256 devices in a mesh: rows: 32 (over z, x), feat: 8 (over y, core).
Axes of the slice: x: 4, y: 4, z: 8, core: 2. Of those that a mesh axis runs over, the one named last changes fastest.
Arguments:
- tile_values: bfloat16 [8192, 512, 128], P('rows', 'feat'), may hold values from -6 to 6
- tile_blocks: int32 [8192, 512], P('rows', 'feat'), may hold values from 0 to 1023
- tile_counts: int32 [8192, 8], P('rows', 'feat'), may hold values from 1 to 64, as said below
- labels: int32 [8192], P('rows'), may hold values 0 or 1
- owner_rank: int32 [8192], P('rows'), may hold values from 0 to 31, as said below
- weights: float32 [8192, 128], P(('feat', 'rows')), may hold values from -0.09375 to 0.09375
Outputs:
- owned_margins: float32 [8192], P('rows')
- gradient: float32 [8192, 128], P(('feat', 'rows'))
- loss: float32 [], replicated
The draws below stay inside these ranges and needn't reach their ends.
Inputs may be any that keep to these rules, and one draw needn't show every extreme that they name: `owner_rank`: within each aligned block of 256 examples, every owner is named by exactly 8 examples. `tile_counts`: in every aligned block of 256 examples, each shard's column holds at least one example with exactly 64 used slots.
All inputs are finite; a program needn't handle non-finite values. No bound on the sum of `labels` on one device may be relied on, other than what follows from the above.
Results may differ from the reference program's by a relative error of at most 0.003.
Values may be sent and summed in bfloat16 or wider, within the bound.
A program may use at most 64 MiB of HBM per device.

```python
import jax
import jax.numpy as jnp
from jax import lax

TILE = 128
EX_DEV = 256
TPAD = 64
EXAMPLES = 8192
SLOTS = 512
NBLK = 8192
BLK_SHARD = 1024
PER_PEER = 8
N_ROWS = 32
N_FEAT = 8


def draw_tile_counts(key, part):
    device_count = EXAMPLES // EX_DEV
    shard_count = SLOTS // TPAD
    key_shift = jax.random.fold_in(key, 11)
    key_value = jax.random.fold_in(key, 12)
    key_full = jax.random.fold_in(key, 13)
    device_of = jnp.arange(EXAMPLES, dtype=jnp.int32) // EX_DEV
    spread = max(device_count - 1, 1)
    ceiling = TPAD * (spread + 2 * device_of) // (3 * spread)
    ceiling = jnp.maximum(ceiling, 1)
    shifts = jax.random.randint(key_shift, (EXAMPLES, shard_count), 0, 4)
    divisor = jnp.left_shift(jnp.ones_like(shifts), shifts)
    upper = jnp.maximum(ceiling[:, None] // divisor, 1)
    raw_value = jax.random.randint(key_value, (EXAMPLES, shard_count), 0, 1048576)
    drawn = raw_value % upper + 1
    chosen = jax.random.randint(key_full, (device_count, shard_count), 0, EX_DEV)
    local_index = jnp.arange(EXAMPLES, dtype=jnp.int32) % EX_DEV
    marked = local_index[:, None] == jnp.repeat(chosen, EX_DEV, axis=0)
    return jnp.where(marked, TPAD, drawn).astype(jnp.int32)


def one_block_owner(block_key):
    return jax.random.permutation(block_key, EX_DEV)


def draw_owner_rank(key, part):
    device_count = EXAMPLES // EX_DEV
    block_keys = jax.random.split(jax.random.fold_in(key, 21), device_count)
    shuffled = jax.vmap(one_block_owner)(block_keys)
    return (shuffled // PER_PEER).reshape(EXAMPLES).astype(jnp.int32)


def set_ends(values, key, smallest, high):
    extent = values.shape
    place = [jax.random.randint(jax.random.fold_in(key, axis), (), 0, extent[axis]) for axis in range(len(extent))]
    values = values.at[tuple(place)].set(smallest)
    longest = extent.index(max(extent))
    place[longest] = (place[longest] + 1) % extent[longest]
    return values.at[tuple(place)].set(high)


def levels(rng, dims, pieces, smallest, largest):
    def one(dim, blocks):
        draws = jax.random.uniform(jax.random.fold_in(jax.random.fold_in(rng, 6), dim), (blocks,), jnp.float32, smallest / len(pieces), largest / len(pieces))
        return jnp.repeat(jnp.exp(draws), dims[dim] // blocks).reshape((-1,) + (1,) * (len(dims) - dim - 1))

    factor_of = one(*pieces[0])
    for cut in pieces[1:]:
        factor_of = factor_of * one(*cut)
    return factor_of


def bell_draw(stream_key, dims, width, bound, cuts=(), held_as=jnp.bfloat16):
    loudness = levels(stream_key, dims, cuts, -0.22, 0.18) if cuts else 1.0
    array = jax.random.normal(stream_key, dims, jnp.float32) * width * loudness
    return jnp.minimum(jnp.maximum(array, -bound), bound).astype(held_as)


def setup_inputs(seed: int = 0) -> dict:
    splits = jax.random.split(jax.random.key(seed), 7)
    return {
        "tile_values": bell_draw(splits[0], (EXAMPLES, SLOTS, TILE), 1.0, 6.0, ((0, 32), (1, 8))),
        "tile_blocks": set_ends(jax.random.randint(splits[1], (EXAMPLES, SLOTS), 0, BLK_SHARD), jax.random.fold_in(splits[1], 1), 0, BLK_SHARD - 1).astype(jnp.int32),
        "tile_counts": draw_tile_counts(jax.random.fold_in(splits[6], 71), 0),
        "labels": set_ends((jax.random.randint(splits[3], (EXAMPLES,), 0, 2) < 1).astype(jnp.int32), jax.random.fold_in(splits[3], 1), 0, 1),
        "owner_rank": draw_owner_rank(jax.random.fold_in(splits[6], 71), 0),
        "weights": bell_draw(splits[5], (NBLK, TILE), (TPAD * TPAD) ** -0.5, 0.09375, ((0, 256),), jnp.float32),
    }


def reference(tile_values, tile_blocks, tile_counts, labels, owner_rank, weights):
    w_half = weights.astype(jnp.bfloat16)
    slot_index = jnp.arange(TPAD, dtype=jnp.int32)

    def shard_pieces(shard_index):
        values = lax.dynamic_slice_in_dim(tile_values, shard_index * TPAD, TPAD, 1)
        block_ids = lax.dynamic_slice_in_dim(tile_blocks, shard_index * TPAD, TPAD, 1)
        used = lax.dynamic_slice_in_dim(tile_counts, shard_index, 1, 1)
        live_slot = slot_index[None, :] < used
        return values, block_ids, live_slot

    def shard_margin(shard_index):
        values, block_ids, live_slot = shard_pieces(shard_index)
        weight_table = lax.dynamic_slice_in_dim(w_half, shard_index * BLK_SHARD, BLK_SHARD, 0)
        picked = weight_table[block_ids]
        products = jnp.sum(values.astype(jnp.float32) * picked.astype(jnp.float32), axis=2)
        return jnp.sum(jnp.where(live_slot, products, jnp.float32(0.0)), axis=1)

    shard_index_all = jnp.arange(N_FEAT, dtype=jnp.int32)
    partials = lax.map(shard_margin, shard_index_all)
    margin = jnp.sum(partials, axis=0)
    label_float = labels.astype(jnp.float32)
    residual = jax.nn.sigmoid(margin) - label_float
    loss = jnp.sum(jax.nn.softplus(margin) - label_float * margin) / EXAMPLES
    resid_half = residual.astype(jnp.bfloat16)

    def shard_gradient(shard_index):
        values, block_ids, live_slot = shard_pieces(shard_index)
        coefficient = jnp.where(live_slot, resid_half[:, None], jnp.zeros((), jnp.bfloat16))
        weighted = values.astype(jnp.float32) * coefficient.astype(jnp.float32)[:, :, None]
        return jax.ops.segment_sum(weighted.reshape(-1, TILE), block_ids.reshape(-1), num_segments=BLK_SHARD)

    gradient = lax.map(shard_gradient, shard_index_all).reshape(NBLK, TILE)
    owners = owner_rank.reshape(N_ROWS, EX_DEV)
    send_order = jnp.argsort(owners, axis=1, stable=True).astype(jnp.int32)
    source = send_order + (jnp.arange(N_ROWS, dtype=jnp.int32) * EX_DEV)[:, None]
    source = jnp.transpose(source.reshape(N_ROWS, N_ROWS, PER_PEER), (1, 0, 2)).reshape(EXAMPLES)
    owned_margins = margin[source]
    return owned_margins, gradient, loss
```

```python
import jax
import jax.numpy as jnp
from jax import lax
from jax.experimental import pallas as pl
from jax.experimental.pallas import tpu as pltpu
from jax.sharding import PartitionSpec as P

MESH = pl.DeviceIdType.MESH
NZ, NX = 8, 4
N_ROWS = NZ * NX
N_FEAT = 8
BF = jnp.bfloat16
F32 = jnp.float32
I16 = jnp.int16
I32 = jnp.int32
PAIRS = 128
GROUP = 8
VCHUNKS = 8


def iota(shape, dim, dtype=I32):
    return lax.broadcasted_iota(I32, shape, dim).astype(dtype)


def body(
    values_hbm, blocks_ref, counts_ref, labels_ref, owner_ref, w_ref,
    own_out, grad_out, loss_out,
    vbuf, vx, onehot, acc, wtab, wcat, cct, qrow, coef, rankhot,
    mbuf, sbuf, rbuf, xrow, gacc, gsend, grecv,
    vsem, zs, zr, xs, xr, ms, mr, os_, or_, gs, gr,
):
    r = lax.axis_index("rows")
    f = lax.axis_index("feat")
    z = r // NX
    x = r % NX

    def row_at(dz, dx):
        return ((z + dz) % NZ) * NX + (x + dx) % NX

    def vcopy(i):
        n = 2 * PAIRS // VCHUNKS
        part = pl.ds(i * n, n)
        return pltpu.make_async_copy(values_hbm.at[part], vbuf.at[part], vsem.at[i])

    for i in range(VCHUNKS // 2):
        vcopy(i).start()
        vcopy(i + VCHUNKS // 2).start()
    wtab[2, 0] = w_ref[...].astype(BF)

    barrier = pltpu.get_barrier_semaphore()
    for dz in range(1, NZ):
        pl.semaphore_signal(barrier, inc=1, device_id={"rows": row_at(dz, 0)}, device_id_type=MESH)
    for dx in range(1, NX):
        pl.semaphore_signal(barrier, inc=1, device_id={"rows": row_at(0, dx)}, device_id_type=MESH)
    for df in range(1, N_FEAT):
        pl.semaphore_signal(barrier, inc=1, device_id={"feat": (f + df) % N_FEAT}, device_id_type=MESH)

    blocks = blocks_ref[...]
    dz2 = (lax.shift_right_logical(blocks, 7) - z + (2 + NZ)) & (NZ - 1)
    dxb = (lax.shift_right_logical(blocks, 5) - x + NX) & (NX - 1)
    stage = lax.shift_right_logical(dz2, 2)
    half = lax.shift_right_logical(dz2, 1) & 1
    code = half * 512 + stage * 256 + (dz2 & 1) * 128 + dxb * 32 + (blocks & 31)
    code = jnp.where(iota(blocks.shape, 1) < counts_ref[...], code, -1)
    pair_code = jnp.concatenate([code[:PAIRS], code[PAIRS:]], axis=1)
    qrow[...] = pair_code & 511
    cct[...] = pair_code.T

    pl.semaphore_wait(barrier, NZ - 1 + NX - 1 + N_FEAT - 1)

    def zcopy(dz):
        slot = (dz + 2) % NZ
        return pltpu.make_async_remote_copy(
            wtab.at[2, 0], wtab.at[slot, 0], zs.at[dz - 1], zr.at[dz - 1],
            device_id={"rows": row_at(NZ - dz, 0)}, device_id_type=MESH)

    def xcopy(slot, dx):
        return pltpu.make_async_remote_copy(
            wtab.at[slot, 0], wtab.at[slot, dx], xs.at[slot, dx - 1], xr.at[slot, dx - 1],
            device_id={"rows": row_at(0, NX - dx)}, device_id_type=MESH)

    for dz in (4, 3, 5, 2, 6, 1, 7):
        zcopy(dz).start()
    for dx in (2, 1, 3):
        xcopy(2, dx).start()

    for h in range(2):
        mine = jnp.broadcast_to(owner_ref[pl.ds(h, 1), :], (PAIRS, PAIRS)).T
        rank = jnp.zeros((PAIRS, 1), F32)
        for g in range(2):
            same = (mine == owner_ref[pl.ds(g, 1), :]) & (
                iota((PAIRS, PAIRS), 1) + g * PAIRS < iota((PAIRS, PAIRS), 0) + h * PAIRS)
            rank = rank + jnp.sum(jnp.where(same, 1.0, 0.0), axis=1, keepdims=True)
        lane = (iota((PAIRS, PAIRS), 1) - 8 * (r % 16)).astype(F32)
        rankhot[pl.ds(h * PAIRS, PAIRS), :] = jnp.where(rank == lane, 1.0, 0.0).astype(BF)

    def build(i, _):
        codes = cct[...]
        for u in range(GROUP):
            k = i * GROUP + u
            wide = jnp.broadcast_to(codes[:, u:u + 1], (PAIRS, PAIRS))
            c16 = wide.astype(I16)
            q16 = (wide & 511).astype(I16)
            rows = pl.ds(pl.multiple_of(k * PAIRS, PAIRS), PAIRS)
            for t in range(4):
                hit = q16 == iota((PAIRS, PAIRS), 1, I16) + jnp.int16(128 * t)
                onehot[rows, t * 128:(t + 1) * 128] = jnp.where(hit, jnp.ones((), BF), jnp.zeros((), BF))
            v = jnp.concatenate([vbuf[k], vbuf[k + PAIRS]], axis=0)
            zero = jnp.zeros((), BF)
            high = c16 >= jnp.int16(512)
            low = c16 >= jnp.int16(0)
            v1 = jnp.where(high, v, zero)
            vx[rows, 0:128] = jnp.where(low, v - v1, zero)
            vx[rows, 128:256] = v1
        cct[...] = pltpu.roll(codes, PAIRS - GROUP, 1)
        return 0

    steps = PAIRS // GROUP
    quarter = steps // 4
    for part, arrivals in enumerate(((1, 7), (2, 6), (3, 5), (4,))):
        vcopy(part).wait()
        vcopy(part + VCHUNKS // 2).wait()
        lax.fori_loop(part * quarter, (part + 1) * quarter, build, 0)
        for dz in arrivals:
            zcopy(dz).wait_recv()
            for dx in (2, 1, 3):
                xcopy((dz + 2) % NZ, dx).start()

    for s in range(2):
        for slot in range(4 * s, 4 * s + 4):
            for dx in range(1, NX):
                xcopy(slot, dx).wait_recv()
        for h in range(2):
            for j in range(2):
                wcat[s, j * 128:(j + 1) * 128, h * 128:(h + 1) * 128] = (
                    wtab[4 * s + 2 * h + j].reshape(128, 128))

        def forward(i, _, s=s):
            rows = pl.ds(pl.multiple_of(i * (GROUP * PAIRS), GROUP * PAIRS), GROUP * PAIRS)
            out = jnp.dot(onehot[rows, s * 256:(s + 1) * 256], wcat[s], preferred_element_type=F32)
            prod = out * vx[rows, :].astype(F32)
            prod = prod[:, :128] + prod[:, 128:]
            prod = prod.reshape(GROUP, 2, 8, 8, 128).sum(axis=2)
            ks = pl.ds(i * GROUP, GROUP)
            if s == 0:
                acc[ks] = prod
            else:
                acc[ks] = acc[ks] + prod
            return 0

        lax.fori_loop(0, steps, forward, 0)

    for h in range(2):
        rows_sum = acc[:, h].sum(axis=1)
        mbuf[f, pl.ds(h, 1), :] = jnp.sum(rows_sum.T, axis=0, keepdims=True)

    def mcopy(df):
        return pltpu.make_async_remote_copy(
            mbuf.at[f], mbuf.at[f], ms.at[df - 1], mr.at[df - 1],
            device_id={"feat": (f + df) % N_FEAT}, device_id_type=MESH)

    def mcopy_in(df):
        src = (f + N_FEAT - df) % N_FEAT
        return pltpu.make_async_remote_copy(
            mbuf.at[src], mbuf.at[src], ms.at[df - 1], mr.at[df - 1],
            device_id={"feat": (f + df) % N_FEAT}, device_id_type=MESH)

    for df in (4, 3, 5, 2, 6, 1, 7):
        mcopy(df).start()
    for df in range(1, N_FEAT):
        mcopy_in(df).wait_recv()
    margin = mbuf[0]
    for i in range(1, N_FEAT):
        margin = margin + mbuf[i]
    label = labels_ref[...].astype(F32)
    residual = 1.0 / (1.0 + jnp.exp(-margin)) - label
    resid_half = residual.astype(BF).astype(F32)
    spread = [jnp.broadcast_to(resid_half[h:h + 1, :], (PAIRS, PAIRS)).T for h in range(2)]
    coef[...] = jnp.where(iota((PAIRS, PAIRS), 1) < 64, spread[0], spread[1])

    def gcopy(slot, dx):
        dz = (slot + NZ - 2) % NZ
        return pltpu.make_async_remote_copy(
            gsend.at[slot, dx], grecv.at[slot, dx], gs.at[slot, dx], gr.at[slot, dx],
            device_id={"rows": row_at(dz, dx)}, device_id_type=MESH)

    def gradient_half(s):
        gacc[...] = jnp.zeros(gacc.shape, F32)

        def step(i, _):
            total = None
            for t in range(GROUP // 2):
                left = []
                for u in range(2):
                    k = i * GROUP + 2 * t + u
                    q16 = jnp.broadcast_to(qrow[pl.ds(k, 1), :], (16, PAIRS)).astype(I16)
                    c16 = jnp.broadcast_to(coef[pl.ds(k, 1), :], (16, PAIRS)).astype(BF)
                    q16 = jnp.concatenate([q16] * 16, axis=0)
                    c16 = jnp.concatenate([c16] * 16, axis=0)
                    hit = q16 == iota((256, PAIRS), 0, I16) + jnp.int16(256 * s)
                    left.append(jnp.where(hit, c16, jnp.zeros((), BF)))
                start = pl.multiple_of((i * GROUP + 2 * t) * PAIRS, 2 * PAIRS)
                d = jnp.dot(jnp.concatenate(left, axis=1), vx[pl.ds(start, 2 * PAIRS), :],
                            preferred_element_type=F32)
                total = d if total is None else total + d
            gacc[...] += total
            return 0

        lax.fori_loop(0, steps, step, 0)

    def send_half(s):
        for j in range(2):
            for h in range(2):
                slot = 4 * s + 2 * h + j
                for dx in range(NX):
                    lo = j * 128 + dx * 32
                    block = gacc[lo:lo + 32, h * 128:(h + 1) * 128]
                    if slot == 2 and dx == 0:
                        grad_out[...] = block
                    else:
                        gsend[slot, dx] = block.astype(BF)
        for slot in ((6, 5, 7, 4) if s else (0, 3, 1, 2)):
            for dx in (2, 1, 3, 0):
                if slot != 2 or dx != 0:
                    gcopy(slot, dx).start()

    gradient_half(1)
    send_half(1)

    loss_terms = jnp.maximum(margin, 0.0) + jnp.log1p(jnp.exp(-jnp.abs(margin))) - label * margin
    loss_here = jnp.sum(jnp.sum(loss_terms, axis=1, keepdims=True), axis=0, keepdims=True)
    ordered = jnp.zeros((N_ROWS, 128), F32)
    left = margin
    for _ in range(3):
        piece = left.astype(BF).astype(F32)
        left = left - piece
        pick = jnp.concatenate(
            [jnp.where(owner_ref[pl.ds(h, 1), :] == iota((N_ROWS, 128), 0), piece[h:h + 1, :], 0.0)
             for h in range(2)], axis=1).astype(BF)
        ordered = ordered + jnp.dot(pick, rankhot[...], preferred_element_type=F32)
    lane_group = lax.shift_right_logical(iota((N_ROWS, 128), 1), 3)
    xrow[...] = jnp.where(lane_group == (r + 1) % 16, loss_here, ordered)
    for d in range(N_ROWS):
        sbuf[d] = xrow[d:d + 1, :]
    rbuf[r] = xrow[pl.ds(r, 1), :]

    def ocopy(i):
        to = row_at(i // NX, i % NX)
        return pltpu.make_async_remote_copy(
            sbuf.at[to], rbuf.at[r], os_.at[i - 1], or_.at[i - 1],
            device_id={"rows": to}, device_id_type=MESH)

    def ocopy_in(i):
        src = row_at(NZ - i // NX, NX - i % NX)
        return pltpu.make_async_remote_copy(
            sbuf.at[src], rbuf.at[src], os_.at[i - 1], or_.at[i - 1],
            device_id={"rows": src}, device_id_type=MESH)

    for i in range(1, N_ROWS):
        ocopy(i).start()

    gradient_half(0)
    send_half(0)

    for i in range(1, N_ROWS):
        ocopy_in(i).wait_recv()
    group1 = lax.shift_right_logical(iota((1, 128), 1), 3)
    loss_sum = jnp.zeros((1, 128), F32)
    for h in range(2):
        mine = jnp.zeros((1, 128), F32)
        for g in range(16):
            row = rbuf[h * 16 + g]
            mine = mine + jnp.where(group1 == g, row, 0.0)
            loss_sum = loss_sum + jnp.where(group1 == (g + 1) % 16, row, 0.0)
        own_out[pl.ds(h, 1), :] = mine
    loss_total = jnp.sum(loss_sum, axis=1, keepdims=True) * (1.0 / (8.0 * 8192.0))
    loss_out[...] = jnp.broadcast_to(loss_total, (1, 128))

    total = grad_out[...]
    for slot in (1, 3, 0, 4, 7, 5, 6, 2):
        for dx in range(NX):
            if slot != 2 or dx != 0:
                gcopy(slot, dx).wait_recv()
                total = total + grecv[slot, dx].astype(F32)
    grad_out[...] = total

    for dz in range(1, NZ):
        zcopy(dz).wait_send()
    for slot in range(NZ):
        for dx in range(1, NX):
            xcopy(slot, dx).wait_send()
    for df in range(1, N_FEAT):
        mcopy(df).wait_send()
    for i in range(1, N_ROWS):
        ocopy(i).wait_send()
    for slot in range(NZ):
        for dx in range(NX):
            if slot != 2 or dx != 0:
                gcopy(slot, dx).wait_send()


def on_device(tile_values, tile_blocks, tile_counts, labels, owner_rank, weights):
    vmem = pl.BlockSpec(memory_space=pltpu.VMEM)
    dma = pltpu.SemaphoreType.DMA
    own, grad, loss = pl.pallas_call(
        body,
        out_shape=(
            jax.ShapeDtypeStruct((2, 128), F32),
            jax.ShapeDtypeStruct((32, 128), F32),
            jax.ShapeDtypeStruct((1, 128), F32),
        ),
        in_specs=[pl.BlockSpec(memory_space=pl.ANY)] + [vmem] * 5,
        out_specs=(vmem, vmem, vmem),
        scratch_shapes=[
            pltpu.VMEM((256, 64, 128), BF),
            pltpu.VMEM((16384, 256), BF),
            pltpu.VMEM((16384, 512), BF),
            pltpu.VMEM((PAIRS, 2, 8, 128), F32),
            pltpu.VMEM((NZ, NX, 32, 128), BF),
            pltpu.VMEM((2, 256, 256), BF),
            pltpu.VMEM((PAIRS, PAIRS), I32),
            pltpu.VMEM((PAIRS, PAIRS), I32),
            pltpu.VMEM((PAIRS, PAIRS), F32),
            pltpu.VMEM((256, 128), BF),
            pltpu.VMEM((N_FEAT, 2, 128), F32),
            pltpu.VMEM((N_ROWS, 1, 128), F32),
            pltpu.VMEM((N_ROWS, 1, 128), F32),
            pltpu.VMEM((N_ROWS, 128), F32),
            pltpu.VMEM((256, 256), F32),
            pltpu.VMEM((NZ, NX, 32, 128), BF),
            pltpu.VMEM((NZ, NX, 32, 128), BF),
            dma((VCHUNKS,)),
            dma((NZ - 1,)), dma((NZ - 1,)),
            dma((NZ, NX - 1)), dma((NZ, NX - 1)),
            dma((N_FEAT - 1,)), dma((N_FEAT - 1,)),
            dma((N_ROWS - 1,)), dma((N_ROWS - 1,)),
            dma((NZ, NX)), dma((NZ, NX)),
        ],
        compiler_params=pltpu.CompilerParams(
            collective_id=0, has_side_effects=True, vmem_limit_bytes=56 * 1024 * 1024),
    )(tile_values, tile_blocks, tile_counts, labels.reshape(2, 128), owner_rank.reshape(2, 128), weights)
    return own.reshape(256), grad, loss[0, 0]


def solution(mesh):
    in_specs = (
        P("rows", "feat", None),
        P("rows", "feat"),
        P("rows", "feat"),
        P("rows"),
        P("rows"),
        P(("feat", "rows"), None),
    )
    out_specs = (P("rows"), P(("feat", "rows"), None), P())
    return jax.shard_map(
        on_device, mesh=mesh, in_specs=in_specs, out_specs=out_specs, check_vma=False
    )
```

```python
import jax
import jax.numpy as jnp
from jax import lax
from jax.experimental import pallas as pl
from jax.experimental.pallas import tpu as pltpu
from jax.sharding import PartitionSpec as P

MESH = pl.DeviceIdType.MESH
NZ, NX = 8, 4
N_ROWS = NZ * NX
N_FEAT = 8
BF = jnp.bfloat16
F32 = jnp.float32
I16 = jnp.int16
I32 = jnp.int32
PAIRS = 128
GROUP = 8
VCHUNKS = 8
FSUB = 8
BSUB = 32


def iota(shape, dim, dtype=I32):
    return lax.broadcasted_iota(I32, shape, dim).astype(dtype)


def body(
    blocks_hbm, counts_hbm, labels_hbm, owner_hbm, w_hbm, values_hbm,
    own_out, grad_out, loss_out,
    blocks_ref, counts_ref, labels_ref, owner_ref, w_ref,
    vbuf, vx, onehot, acc, wtab, cct, qrow, coef, rankhot,
    mbuf, sbuf, rbuf, xrow, gacc, gsend, grecv,
    isem, vsem, zs, zr, xs, xr, ms, mr, os_, or_, gs, gr,
):
    r = lax.axis_index("rows")
    f = lax.axis_index("feat")
    z = lax.div(r, NX)
    x = lax.rem(r, NX)

    def row_at(dz, dx):
        return lax.rem(z + dz, NZ) * NX + lax.rem(x + dx, NX)

    def feat_at(df):
        return lax.rem(f + df, N_FEAT)

    def stage_of(dz):
        return ((dz + 2) % NZ) // 4

    barrier = pltpu.get_barrier_semaphore()
    for dz in (4, 3, 5, 2, 6, 1, 7):
        pl.semaphore_signal(barrier, inc=1, device_id={"rows": row_at(dz, 0)}, device_id_type=MESH)
    for dx in (2, 1, 3):
        pl.semaphore_signal(barrier, inc=1, device_id={"rows": row_at(0, dx)}, device_id_type=MESH)
    for df in range(1, N_FEAT):
        pl.semaphore_signal(barrier, inc=1, device_id={"feat": feat_at(df)}, device_id_type=MESH)

    fetched = [
        pltpu.make_async_copy(src, dst, isem.at[i])
        for i, (src, dst) in enumerate((
            (w_hbm, w_ref), (blocks_hbm, blocks_ref), (counts_hbm, counts_ref),
            (owner_hbm, owner_ref), (labels_hbm, labels_ref)))
    ]
    for copy in fetched:
        copy.start()

    def vcopy(i):
        n = 2 * PAIRS // VCHUNKS
        part = pl.ds(i * n, n)
        return pltpu.make_async_copy(values_hbm.at[part], vbuf.at[part], vsem.at[i])

    for i in range(VCHUNKS // 2):
        vcopy(i).start()
        vcopy(i + VCHUNKS // 2).start()

    fetched[0].wait()
    wtab[0, 0, 0] = w_ref[...].astype(BF)
    pl.semaphore_wait(barrier, NZ - 1 + NX - 1 + N_FEAT - 1)

    def zcopy(dz):
        return pltpu.make_async_remote_copy(
            wtab.at[0, 0, 0], wtab.at[stage_of(dz), 0, dz % 4], zs, zr.at[dz - 1],
            device_id={"rows": row_at(NZ - dz, 0)}, device_id_type=MESH)

    def xcopy(dz, dx):
        s, q = stage_of(dz), dz % 4
        return pltpu.make_async_remote_copy(
            wtab.at[s, 0, q], wtab.at[s, dx, q], xs, xr.at[s],
            device_id={"rows": row_at(0, NX - dx)}, device_id_type=MESH)

    def all_of(ref, send_sem, recv_sem):
        return pltpu.make_async_remote_copy(
            ref, ref, send_sem, recv_sem, device_id={"rows": row_at(0, 1)}, device_id_type=MESH)

    for dz in (4, 3, 5, 2, 6, 1, 7):
        zcopy(dz).start()
    for dx in (2, 1, 3):
        xcopy(0, dx).start()

    def pass_on(*arrivals):
        for dz in arrivals:
            zcopy(dz).wait_recv()
            for dx in (2, 1, 3):
                xcopy(dz, dx).start()

    fetched[1].wait()
    fetched[2].wait()
    blocks = blocks_ref[...]
    dz = (lax.shift_right_logical(blocks, 7) - z + NZ) & (NZ - 1)
    dx = (lax.shift_right_logical(blocks, 5) - x + NX) & (NX - 1)
    stage = lax.shift_right_logical(dz + 2, 2) & 1
    code = ((lax.shift_right_logical(dz, 1) & 1) * 512 + stage * 256 + dx * 64
            + (dz & 1) * 32 + (blocks & 31))
    code = jnp.where(iota(blocks.shape, 0) < counts_ref[...], code, -1)
    cct[...] = jnp.concatenate([code[:, :PAIRS], code[:, PAIRS:]], axis=0)

    def build(i, _):
        codes = cct[...]
        for u in range(GROUP):
            k = i * GROUP + u
            wide = jnp.broadcast_to(codes[:, u:u + 1], (PAIRS, PAIRS))
            c16 = wide.astype(I16)
            q16 = (wide & 511).astype(I16)
            rows = pl.ds(pl.multiple_of(k * PAIRS, PAIRS), PAIRS)
            for t in range(4):
                hit = q16 == iota((PAIRS, PAIRS), 1, I16) + jnp.int16(128 * t)
                onehot[t, rows, :] = jnp.where(hit, jnp.ones((), BF), jnp.zeros((), BF))
            v = jnp.concatenate([vbuf[k], vbuf[k + PAIRS]], axis=0)
            zero = jnp.zeros((), BF)
            v1 = jnp.where(c16 >= jnp.int16(512), v, zero)
            vx[0, rows, :] = jnp.where(c16 >= jnp.int16(0), v - v1, zero)
            vx[1, rows, :] = v1
        cct[...] = pltpu.roll(codes, PAIRS - GROUP, 1)
        return 0

    steps = PAIRS // GROUP
    quarter = steps // 4
    for part in range(4):
        vcopy(part).wait()
        vcopy(part + VCHUNKS // 2).wait()
        lax.fori_loop(part * quarter, (part + 1) * quarter, build, 0)
        if part == 1:
            pass_on(1, 7)
        if part == 3:
            pass_on(2, 6)
    qrow[...] = (cct[...] & 511).T

    fetched[3].wait()
    fetched[4].wait()
    for h in range(2):
        mine = jnp.broadcast_to(owner_ref[pl.ds(h, 1), :], (PAIRS, PAIRS)).T
        rank = jnp.zeros((PAIRS, 1), F32)
        for g in range(2):
            same = (mine == owner_ref[pl.ds(g, 1), :]) & (
                iota((PAIRS, PAIRS), 1) + g * PAIRS < iota((PAIRS, PAIRS), 0) + h * PAIRS)
            rank = rank + jnp.sum(jnp.where(same, 1.0, 0.0), axis=1, keepdims=True)
        lane = (iota((PAIRS, PAIRS), 1) - 8 * lax.rem(r, 16)).astype(F32)
        rankhot[pl.ds(h * PAIRS, PAIRS), :] = jnp.where(rank == lane, 1.0, 0.0).astype(BF)
    pass_on(3, 5, 4)

    for s in range(2):
        all_of(wtab.at[s, pl.ds(1, NX - 1)], xs, xr.at[s]).wait_recv()
        table = jnp.concatenate(
            [wtab[s, :, pl.ds(2 * h, 2)].reshape(256, 128) for h in range(2)], axis=1)

        def forward(i, _, s=s, table=table):
            for u in range(FSUB):
                k0 = (i * FSUB + u) * GROUP
                rows = pl.ds(pl.multiple_of(k0 * PAIRS, GROUP * PAIRS), GROUP * PAIRS)
                hot = jnp.concatenate([onehot[2 * s, rows, :], onehot[2 * s + 1, rows, :]], axis=1)
                out = jnp.dot(hot, table, preferred_element_type=F32)
                prod = out[:, :128] * vx[0, rows, :].astype(F32) + out[:, 128:] * vx[1, rows, :].astype(F32)
                prod = prod.reshape(GROUP, 2, 8, 8, 128).sum(axis=2)
                for h in range(2):
                    ks = pl.ds(pl.multiple_of(k0 * 8, 8 * GROUP), 8 * GROUP)
                    part = prod[:, h].reshape(8 * GROUP, 128)
                    if s == 0:
                        acc[h, ks, :] = part
                    else:
                        acc[h, ks, :] = acc[h, ks, :] + part
            return 0

        lax.fori_loop(0, steps // FSUB, forward, 0)

    for h in range(2):
        groups = []
        for g in range(PAIRS // 8):
            total = acc[h, pl.ds(64 * g, 8, stride=8), :]
            for i in range(1, 8):
                total = total + acc[h, pl.ds(64 * g + i, 8, stride=8), :]
            groups.append(total)
        rows_sum = jnp.concatenate(groups, axis=0)
        mbuf[f, pl.ds(h, 1), :] = jnp.sum(rows_sum.T, axis=0, keepdims=True)
    for df in (4, 3, 5, 2, 6, 1, 7):
        pltpu.make_async_remote_copy(
            mbuf.at[f], mbuf.at[f], ms, mr,
            device_id={"feat": feat_at(df)}, device_id_type=MESH).start()
    all_of(mbuf.at[pl.ds(0, N_FEAT - 1)], ms, mr).wait_recv()
    margin = mbuf[0]
    for i in range(1, N_FEAT):
        margin = margin + mbuf[i]
    label = labels_ref[...].astype(F32)
    residual = 1.0 / (1.0 + jnp.exp(-margin)) - label
    resid_half = residual.astype(BF).astype(F32)
    spread = [jnp.broadcast_to(resid_half[h:h + 1, :], (PAIRS, PAIRS)).T for h in range(2)]
    coef[...] = jnp.where(iota((PAIRS, PAIRS), 1) < 64, spread[0], spread[1])

    def gradient_half(s):
        def step(i, _):
            total = None
            for t in range(BSUB):
                left = []
                for u in range(2):
                    k = (i * BSUB + t) * 2 + u
                    q16 = jnp.broadcast_to(qrow[pl.ds(k, 1), :], (16, PAIRS)).astype(I16)
                    c16 = jnp.broadcast_to(coef[pl.ds(k, 1), :], (16, PAIRS)).astype(BF)
                    q16 = jnp.concatenate([q16] * 16, axis=0)
                    c16 = jnp.concatenate([c16] * 16, axis=0)
                    hit = q16 == iota((256, PAIRS), 0, I16) + jnp.int16(256 * s)
                    left.append(jnp.where(hit, c16, jnp.zeros((), BF)))
                rows = pl.ds(pl.multiple_of((i * BSUB + t) * 2 * PAIRS, 2 * PAIRS), 2 * PAIRS)
                right = jnp.concatenate([vx[0, rows, :], vx[1, rows, :]], axis=1)
                d = jnp.dot(jnp.concatenate(left, axis=1), right, preferred_element_type=F32)
                total = d if total is None else total + d
            for h in range(2):
                gacc[h] = gacc[h] + total[:, 128 * h:128 * h + 128]
            return 0

        gacc[...] = jnp.zeros(gacc.shape, F32)
        lax.fori_loop(0, PAIRS // 2 // BSUB, step, 0)
        for h in range(2):
            for j in range(2):
                for dx in range(NX):
                    block = gacc[h, pl.ds(dx * 64 + j * 32, 32), :]
                    if s == 0 and h == 0 and j == 0 and dx == 0:
                        grad_out[...] = block
                    else:
                        gsend[s, dx * 4 + 2 * h + j] = block.astype(BF)
        for dz in ((4, 3, 5, 2) if s else (6, 7, 1, 0)):
            for dx in (2, 1, 3, 0):
                if dz != 0 or dx != 0:
                    n = dx * 4 + dz % 4
                    pltpu.make_async_remote_copy(
                        gsend.at[s, n], grecv.at[s, n], gs.at[s], gr.at[s],
                        device_id={"rows": row_at(dz, dx)}, device_id_type=MESH).start()

    gradient_half(1)

    loss_terms = jnp.maximum(margin, 0.0) + jnp.log1p(jnp.exp(-jnp.abs(margin))) - label * margin
    loss_here = jnp.sum(jnp.sum(loss_terms, axis=1, keepdims=True), axis=0, keepdims=True)
    ordered = jnp.zeros((N_ROWS, 128), F32)
    left = margin
    for _ in range(3):
        piece = left.astype(BF).astype(F32)
        left = left - piece
        pick = jnp.concatenate(
            [jnp.where(owner_ref[pl.ds(h, 1), :] == iota((N_ROWS, 128), 0), piece[h:h + 1, :], 0.0)
             for h in range(2)], axis=1).astype(BF)
        ordered = ordered + jnp.dot(pick, rankhot[...], preferred_element_type=F32)
    lane_group = lax.shift_right_logical(iota((N_ROWS, 128), 1), 3)
    xrow[...] = jnp.where(lane_group == lax.rem(r + 1, 16), loss_here, ordered)
    for d in range(N_ROWS):
        sbuf[d] = xrow[d:d + 1, :]
    rbuf[r] = xrow[pl.ds(r, 1), :]
    for i in range(1, N_ROWS):
        to = row_at(i // NX, i % NX)
        pltpu.make_async_remote_copy(
            sbuf.at[to], rbuf.at[r], os_, or_,
            device_id={"rows": to}, device_id_type=MESH).start()

    gradient_half(0)

    all_of(rbuf.at[pl.ds(0, N_ROWS - 1)], os_, or_).wait_recv()
    group1 = lax.shift_right_logical(iota((1, 128), 1), 3)
    loss_sum = jnp.zeros((1, 128), F32)
    for h in range(2):
        mine = jnp.zeros((1, 128), F32)
        for g in range(16):
            row = rbuf[h * 16 + g]
            mine = mine + jnp.where(group1 == g, row, 0.0)
            loss_sum = loss_sum + jnp.where(group1 == (g + 1) % 16, row, 0.0)
        own_out[pl.ds(h, 1), :] = mine
    loss_total = jnp.sum(loss_sum, axis=1, keepdims=True) * (1.0 / (8.0 * 8192.0))
    loss_out[...] = jnp.broadcast_to(loss_total, (1, 128))

    total = grad_out[...]
    all_of(grecv.at[1], gs.at[1], gr.at[1]).wait_recv()
    for n in range(16):
        total = total + grecv[1, n].astype(F32)
    all_of(grecv.at[0, pl.ds(1, 15)], gs.at[0], gr.at[0]).wait_recv()
    for n in range(1, 16):
        total = total + grecv[0, n].astype(F32)
    grad_out[...] = total

    all_of(gsend.at[0, pl.ds(0, NZ - 1)], zs, zr.at[0]).wait_send()
    all_of(wtab.at[pl.ds(0, 2), pl.ds(1, NX - 1)], xs, xr.at[0]).wait_send()
    all_of(mbuf.at[pl.ds(0, N_FEAT - 1)], ms, mr).wait_send()
    all_of(sbuf.at[pl.ds(0, N_ROWS - 1)], os_, or_).wait_send()
    all_of(gsend.at[1], gs.at[1], gr.at[1]).wait_send()
    all_of(gsend.at[0, pl.ds(1, 15)], gs.at[0], gr.at[0]).wait_send()


def on_device(tile_values, tile_blocks, tile_counts, labels, owner_rank, weights):
    vmem = pl.BlockSpec(memory_space=pltpu.VMEM)
    dma = pltpu.SemaphoreType.DMA
    own, grad, loss = pl.pallas_call(
        body,
        out_shape=(
            jax.ShapeDtypeStruct((2, 128), F32),
            jax.ShapeDtypeStruct((32, 128), F32),
            jax.ShapeDtypeStruct((1, 128), F32),
        ),
        in_specs=[pl.BlockSpec(memory_space=pl.ANY)] * 6,
        out_specs=(vmem, vmem, vmem),
        scratch_shapes=[
            pltpu.VMEM((64, 256), I32),
            pltpu.VMEM((1, 256), I32),
            pltpu.VMEM((2, 128), I32),
            pltpu.VMEM((2, 128), I32),
            pltpu.VMEM((32, 128), F32),
            pltpu.VMEM((256, 64, 128), BF),
            pltpu.VMEM((2, 16384, 128), BF),
            pltpu.VMEM((4, 16384, 128), BF),
            pltpu.VMEM((2, PAIRS * 8, 128), F32),
            pltpu.VMEM((2, NX, 4, 32, 128), BF),
            pltpu.VMEM((PAIRS, PAIRS), I32),
            pltpu.VMEM((PAIRS, PAIRS), I32),
            pltpu.VMEM((PAIRS, PAIRS), F32),
            pltpu.VMEM((256, 128), BF),
            pltpu.VMEM((N_FEAT, 2, 128), F32),
            pltpu.VMEM((N_ROWS, 1, 128), F32),
            pltpu.VMEM((N_ROWS, 1, 128), F32),
            pltpu.VMEM((N_ROWS, 128), F32),
            pltpu.VMEM((2, 256, 128), F32),
            pltpu.VMEM((2, 16, 32, 128), BF),
            pltpu.VMEM((2, 16, 32, 128), BF),
            dma((5,)), dma((VCHUNKS,)),
            dma, dma((NZ - 1,)),
            dma, dma((2,)),
            dma, dma,
            dma, dma,
            dma((2,)), dma((2,)),
        ],
        compiler_params=pltpu.CompilerParams(
            collective_id=0, has_side_effects=True, vmem_limit_bytes=56 * 1024 * 1024),
    )(tile_blocks.T, tile_counts.T, labels.reshape(2, 128), owner_rank.reshape(2, 128), weights, tile_values)
    return own.reshape(256), grad, loss[0, 0]


def solution(mesh):
    in_specs = (
        P("rows", "feat", None),
        P("rows", "feat"),
        P("rows", "feat"),
        P("rows"),
        P("rows"),
        P(("feat", "rows"), None),
    )
    out_specs = (P("rows"), P(("feat", "rows"), None), P())
    return jax.shard_map(
        on_device, mesh=mesh, in_specs=in_specs, out_specs=out_specs, check_vma=False
    )
```

```python
import jax
import jax.numpy as jnp
from jax import lax
from jax.experimental import pallas as pl
from jax.experimental.pallas import tpu as pltpu
from jax.sharding import PartitionSpec as P

MESH = pl.DeviceIdType.MESH
NZ, NX = 8, 4
N_ROWS = NZ * NX
N_FEAT = 8
BF = jnp.bfloat16
F32 = jnp.float32
I16 = jnp.int16
I32 = jnp.int32
PAIRS = 128
GROUP = 8
VCHUNKS = 8
FSUB = 8


def iota(shape, dim, dtype=I32):
    return lax.broadcasted_iota(I32, shape, dim).astype(dtype)


def body(
    blocks_hbm, counts_hbm, labels_hbm, owner_hbm, w_hbm, values_hbm,
    own_out, grad_out, loss_out,
    blocks_ref, counts_ref, labels_ref, owner_ref, w_ref,
    vbuf, vx, onehot, acc, wtab, cct, qrow, coef, rankhot,
    mbuf, sbuf, rbuf, xrow, gsend, grecv,
    isem, vsem, zs, zr, xs, xr, ms, mr, os_, or_, gs, gr,
):
    r = lax.axis_index("rows")
    f = lax.axis_index("feat")
    z = lax.div(r, NX)
    x = lax.rem(r, NX)

    def row_at(dz, dx):
        return lax.rem(z + dz, NZ) * NX + lax.rem(x + dx, NX)

    def feat_at(df):
        return lax.rem(f + df, N_FEAT)

    def place(dz):
        return ((dz + 2) // 4) % 2, dz // 4, ((dz + 1) // 2) % 2

    fetched = [
        pltpu.make_async_copy(src, dst, isem.at[i])
        for i, (src, dst) in enumerate((
            (w_hbm, w_ref), (blocks_hbm, blocks_ref), (counts_hbm, counts_ref),
            (owner_hbm, owner_ref), (labels_hbm, labels_ref)))
    ]
    for copy in fetched:
        copy.start()

    def vcopy(i):
        n = 2 * PAIRS // VCHUNKS
        part = pl.ds(i * n, n)
        return pltpu.make_async_copy(values_hbm.at[part], vbuf.at[part], vsem.at[i])

    for i in range(VCHUNKS // 2):
        vcopy(i).start()
        vcopy(i + VCHUNKS // 2).start()

    barrier = pltpu.get_barrier_semaphore()
    for dz in (2, 6, 1, 7):
        pl.semaphore_signal(barrier, inc=1, device_id={"rows": row_at(dz, 0)}, device_id_type=MESH)
    for dx in (2, 1, 3):
        pl.semaphore_signal(barrier, inc=1, device_id={"rows": row_at(0, dx)}, device_id_type=MESH)
    for df in range(1, N_FEAT):
        pl.semaphore_signal(barrier, inc=1, device_id={"feat": feat_at(df)}, device_id_type=MESH)

    fetched[0].wait()
    wtab[0, 0, 0, 0] = w_ref[...].astype(BF)
    pl.semaphore_wait(barrier, 4 + NX - 1 + N_FEAT - 1)

    def slot(dz, dx):
        return wtab.at[(*place(dz), dx)]

    def zcopy(dz):
        return pltpu.make_async_remote_copy(
            slot(0, 0), slot(dz, 0), zs, zr.at[dz],
            device_id={"rows": row_at(NZ - dz, 0)}, device_id_type=MESH)

    def xcopy(dz, dx, recv_sem):
        return pltpu.make_async_remote_copy(
            slot(dz, 0), slot(dz, dx), xs, recv_sem,
            device_id={"rows": row_at(0, NX - dx)}, device_id_type=MESH)

    def relay(dz, step, dx):
        return pltpu.make_async_remote_copy(
            slot(dz, 0), slot(dz + step, dx), xs, xr.at[1],
            device_id={"rows": row_at(NZ - step, NX - dx)}, device_id_type=MESH)

    def all_of(ref, send_sem, recv_sem):
        return pltpu.make_async_remote_copy(
            ref, ref, send_sem, recv_sem, device_id={"rows": row_at(0, 1)}, device_id_type=MESH)

    for dz in (2, 6, 1, 7):
        zcopy(dz).start()
    for dx in (2, 1, 3):
        xcopy(0, dx, xr.at[2]).start()

    def pass_on():
        for dz in (1, 7, 2, 6):
            zcopy(dz).wait_recv()
            for dx in (2, 1, 3):
                xcopy(dz, dx, xr.at[place(dz)[0]]).start()
        all_of(gsend.at[0, pl.ds(0, 3)], xs, xr.at[2]).wait_recv()
        for dx in (2, 1, 3, 0):
            relay(2, 2, dx).start()
        for dx in (2, 1, 3, 0):
            relay(2, 1, dx).start()
            relay(6, -1, dx).start()

    fetched[1].wait()
    fetched[2].wait()
    blocks = blocks_ref[...]
    dz = (lax.shift_right_logical(blocks, 7) - z + NZ) & (NZ - 1)
    dx = (lax.shift_right_logical(blocks, 5) - x + NX) & (NX - 1)
    stage = lax.shift_right_logical(dz + 2, 2) & 1
    piece = lax.shift_right_logical(dz + 1, 1) & 1
    code = lax.shift_right_logical(dz, 2) * 512 + stage * 256 + piece * 128 + dx * 32 + (blocks & 31)
    code = jnp.where(iota(blocks.shape, 0) < counts_ref[...], code, -1)
    cct[...] = jnp.concatenate([code[:, :PAIRS], code[:, PAIRS:]], axis=0)

    def build(i, _):
        codes = cct[...]
        for u in range(GROUP):
            k = i * GROUP + u
            wide = jnp.broadcast_to(codes[:, u:u + 1], (PAIRS, PAIRS))
            c16 = wide.astype(I16)
            q16 = (wide & 511).astype(I16)
            rows = pl.ds(pl.multiple_of(k * PAIRS, PAIRS), PAIRS)
            for t in range(4):
                hit = q16 == iota((PAIRS, PAIRS), 1, I16) + jnp.int16(128 * t)
                onehot[t, rows, :] = jnp.where(hit, jnp.ones((), BF), jnp.zeros((), BF))
            v = jnp.concatenate([vbuf[k], vbuf[k + PAIRS]], axis=0)
            zero = jnp.zeros((), BF)
            v1 = jnp.where(c16 >= jnp.int16(512), v, zero)
            vx[0, rows, :] = jnp.where(c16 >= jnp.int16(0), v - v1, zero)
            vx[1, rows, :] = v1
        cct[...] = pltpu.roll(codes, PAIRS - GROUP, 1)
        return 0

    steps = PAIRS // GROUP
    quarter = steps // 4
    for part in range(4):
        vcopy(part).wait()
        vcopy(part + VCHUNKS // 2).wait()
        lax.fori_loop(part * quarter, (part + 1) * quarter, build, 0)
        if part == 1:
            pass_on()
    qrow[...] = (cct[...] & 511).T

    fetched[3].wait()
    fetched[4].wait()
    for h in range(2):
        mine = jnp.broadcast_to(owner_ref[pl.ds(h, 1), :], (PAIRS, PAIRS)).T
        rank = jnp.zeros((PAIRS, 1), F32)
        for g in range(2):
            same = (mine == owner_ref[pl.ds(g, 1), :]) & (
                iota((PAIRS, PAIRS), 1) + g * PAIRS < iota((PAIRS, PAIRS), 0) + h * PAIRS)
            rank = rank + jnp.sum(jnp.where(same, 1.0, 0.0), axis=1, keepdims=True)
        lane = (iota((PAIRS, PAIRS), 1) - 8 * lax.rem(r, 16)).astype(F32)
        rankhot[pl.ds(h * PAIRS, PAIRS), :] = jnp.where(rank == lane, 1.0, 0.0).astype(BF)

    for s in range(2):
        all_of(gsend.at[pl.ds(0, 3), pl.ds(0, 5 if s else 3)], xs, xr.at[s]).wait_recv()
        table = jnp.concatenate([wtab[s, h].reshape(256, 128) for h in range(2)], axis=1)

        def forward(i, _, s=s, table=table):
            for u in range(FSUB):
                k0 = (i * FSUB + u) * GROUP
                rows = pl.ds(pl.multiple_of(k0 * PAIRS, GROUP * PAIRS), GROUP * PAIRS)
                hot = jnp.concatenate([onehot[2 * s, rows, :], onehot[2 * s + 1, rows, :]], axis=1)
                out = jnp.dot(hot, table, preferred_element_type=F32)
                prod = out[:, :128] * vx[0, rows, :].astype(F32) + out[:, 128:] * vx[1, rows, :].astype(F32)
                prod = prod.reshape(GROUP, 2, 8, 8, 128).sum(axis=2)
                for h in range(2):
                    ks = pl.ds(pl.multiple_of(k0 * 8, 8 * GROUP), 8 * GROUP)
                    part = prod[:, h].reshape(8 * GROUP, 128)
                    if s == 0:
                        acc[h, ks, :] = part
                    else:
                        acc[h, ks, :] = acc[h, ks, :] + part
            return 0

        lax.fori_loop(0, steps // FSUB, forward, 0)

    for h in range(2):
        groups = []
        for g in range(PAIRS // 8):
            total = acc[h, pl.ds(64 * g, 8, stride=8), :]
            for i in range(1, 8):
                total = total + acc[h, pl.ds(64 * g + i, 8, stride=8), :]
            groups.append(total)
        rows_sum = jnp.concatenate(groups, axis=0)
        mbuf[f, pl.ds(h, 1), :] = jnp.sum(rows_sum.T, axis=0, keepdims=True)
    for df in (4, 3, 5, 2, 6, 1, 7):
        pltpu.make_async_remote_copy(
            mbuf.at[f], mbuf.at[f], ms, mr,
            device_id={"feat": feat_at(df)}, device_id_type=MESH).start()
    all_of(mbuf.at[pl.ds(0, N_FEAT - 1)], ms, mr).wait_recv()
    margin = mbuf[0]
    for i in range(1, N_FEAT):
        margin = margin + mbuf[i]
    label = labels_ref[...].astype(F32)
    residual = 1.0 / (1.0 + jnp.exp(-margin)) - label
    resid_half = residual.astype(BF).astype(F32)
    spread = [jnp.broadcast_to(resid_half[h:h + 1, :], (PAIRS, PAIRS)).T for h in range(2)]
    coef[...] = jnp.where(iota((PAIRS, PAIRS), 1) < 64, spread[0], spread[1])

    def gradient_piece(s, j):
        p = 2 * s + j
        total = None
        for t in range(PAIRS // 2):
            left = []
            for u in range(2):
                k = 2 * t + u
                q16 = jnp.broadcast_to(qrow[k:k + 1, :], (16, PAIRS)).astype(I16)
                c16 = jnp.broadcast_to(coef[k:k + 1, :], (16, PAIRS)).astype(BF)
                q16 = jnp.concatenate([q16] * 8, axis=0)
                c16 = jnp.concatenate([c16] * 8, axis=0)
                hit = q16 == iota((128, PAIRS), 0, I16) + jnp.int16(128 * p)
                left.append(jnp.where(hit, c16, jnp.zeros((), BF)))
            rows = pl.ds(t * 2 * PAIRS, 2 * PAIRS)
            right = jnp.concatenate([vx[0, rows, :], vx[1, rows, :]], axis=1)
            d = jnp.dot(jnp.concatenate(left, axis=1), right, preferred_element_type=F32)
            total = d if total is None else total + d
        for h in range(2):
            for dx in range(NX):
                block = total[dx * 32:dx * 32 + 32, 128 * h:128 * h + 128]
                if p == 0 and h == 0 and dx == 0:
                    grad_out[...] = block
                else:
                    gsend[p, h * 4 + dx] = block.astype(BF)
        for dz in range(NZ):
            if place(dz)[0] == s and place(dz)[2] == j:
                for dx in (2, 1, 3, 0):
                    if dz != 0 or dx != 0:
                        n = dz // 4 * 4 + dx
                        pltpu.make_async_remote_copy(
                            gsend.at[p, n], grecv.at[p, n], gs.at[p], gr.at[p],
                            device_id={"rows": row_at(dz, dx)}, device_id_type=MESH).start()

    gradient_piece(1, 0)
    gradient_piece(1, 1)

    loss_terms = jnp.maximum(margin, 0.0) + jnp.log1p(jnp.exp(-jnp.abs(margin))) - label * margin
    loss_here = jnp.sum(jnp.sum(loss_terms, axis=1, keepdims=True), axis=0, keepdims=True)
    ordered = jnp.zeros((N_ROWS, 128), F32)
    left = margin
    for _ in range(3):
        piece = left.astype(BF).astype(F32)
        left = left - piece
        pick = jnp.concatenate(
            [jnp.where(owner_ref[pl.ds(h, 1), :] == iota((N_ROWS, 128), 0), piece[h:h + 1, :], 0.0)
             for h in range(2)], axis=1).astype(BF)
        ordered = ordered + jnp.dot(pick, rankhot[...], preferred_element_type=F32)
    lane_group = lax.shift_right_logical(iota((N_ROWS, 128), 1), 3)
    xrow[...] = jnp.where(lane_group == lax.rem(r + 1, 16), loss_here, ordered)
    for d in range(N_ROWS):
        sbuf[d] = xrow[d:d + 1, :]
    rbuf[r] = xrow[pl.ds(r, 1), :]
    for i in range(1, N_ROWS):
        to = row_at(i // NX, i % NX)
        pltpu.make_async_remote_copy(
            sbuf.at[to], rbuf.at[r], os_, or_,
            device_id={"rows": to}, device_id_type=MESH).start()

    gradient_piece(0, 1)
    gradient_piece(0, 0)

    all_of(rbuf.at[pl.ds(0, N_ROWS - 1)], os_, or_).wait_recv()
    group1 = lax.shift_right_logical(iota((1, 128), 1), 3)
    loss_sum = jnp.zeros((1, 128), F32)
    for h in range(2):
        mine = jnp.zeros((1, 128), F32)
        for g in range(16):
            row = rbuf[h * 16 + g]
            mine = mine + jnp.where(group1 == g, row, 0.0)
            loss_sum = loss_sum + jnp.where(group1 == (g + 1) % 16, row, 0.0)
        own_out[pl.ds(h, 1), :] = mine
    loss_total = jnp.sum(loss_sum, axis=1, keepdims=True) * (1.0 / (8.0 * 8192.0))
    loss_out[...] = jnp.broadcast_to(loss_total, (1, 128))

    total = grad_out[...]
    for p in (2, 3, 1, 0):
        first = 0 if p else 1
        all_of(grecv.at[p, pl.ds(first, 8 - first)], gs.at[p], gr.at[p]).wait_recv()
        for n in range(first, 8):
            total = total + grecv[p, n].astype(F32)
    grad_out[...] = total

    all_of(gsend.at[0, pl.ds(0, 4)], zs, zr.at[0]).wait_send()
    all_of(vx.at[0, pl.ds(0, 27 * 32)], xs, xr.at[0]).wait_send()
    all_of(mbuf.at[pl.ds(0, N_FEAT - 1)], ms, mr).wait_send()
    all_of(sbuf.at[pl.ds(0, N_ROWS - 1)], os_, or_).wait_send()
    for p in range(4):
        first = 0 if p else 1
        all_of(gsend.at[p, pl.ds(first, 8 - first)], gs.at[p], gr.at[p]).wait_send()


def finish(own_in, grad_in, loss_in, own_out, grad_out, loss_out):
    own_out[...] = own_in[...]
    grad_out[...] = grad_in[...]
    loss_out[...] = loss_in[...]


def on_device(tile_values, tile_blocks, tile_counts, labels, owner_rank, weights):
    vmem = pl.BlockSpec(memory_space=pltpu.VMEM)
    dma = pltpu.SemaphoreType.DMA
    results = (
        jax.ShapeDtypeStruct((2, 128), F32),
        jax.ShapeDtypeStruct((32, 128), F32),
        jax.ShapeDtypeStruct((1, 128), F32),
    )
    parts = pl.pallas_call(
        body,
        out_shape=results,
        in_specs=[pl.BlockSpec(memory_space=pl.ANY)] * 6,
        out_specs=(vmem, vmem, vmem),
        scratch_shapes=[
            pltpu.VMEM((64, 256), I32),
            pltpu.VMEM((1, 256), I32),
            pltpu.VMEM((2, 128), I32),
            pltpu.VMEM((2, 128), I32),
            pltpu.VMEM((32, 128), F32),
            pltpu.VMEM((256, 64, 128), BF),
            pltpu.VMEM((2, 16384, 128), BF),
            pltpu.VMEM((4, 16384, 128), BF),
            pltpu.VMEM((2, PAIRS * 8, 128), F32),
            pltpu.VMEM((2, 2, 2, NX, 32, 128), BF),
            pltpu.VMEM((PAIRS, PAIRS), I32),
            pltpu.VMEM((PAIRS, PAIRS), I32),
            pltpu.VMEM((PAIRS, PAIRS), F32),
            pltpu.VMEM((256, 128), BF),
            pltpu.VMEM((N_FEAT, 2, 128), F32),
            pltpu.VMEM((N_ROWS, 1, 128), F32),
            pltpu.VMEM((N_ROWS, 1, 128), F32),
            pltpu.VMEM((N_ROWS, 128), F32),
            pltpu.VMEM((4, 8, 32, 128), BF),
            pltpu.VMEM((4, 8, 32, 128), BF),
            dma((5,)), dma((VCHUNKS,)),
            dma, dma((NZ,)),
            dma, dma((3,)),
            dma, dma,
            dma, dma,
            dma((4,)), dma((4,)),
        ],
        compiler_params=pltpu.CompilerParams(
            collective_id=0, has_side_effects=True, vmem_limit_bytes=56 * 1024 * 1024),
    )(tile_blocks.T, tile_counts.T, labels.reshape(2, 128), owner_rank.reshape(2, 128), weights, tile_values)
    own, grad, loss = pl.pallas_call(
        finish, out_shape=results, in_specs=[vmem] * 3, out_specs=(vmem, vmem, vmem),
    )(*parts)
    return own.reshape(256), grad, loss[0, 0]


def solution(mesh):
    in_specs = (
        P("rows", "feat", None),
        P("rows", "feat"),
        P("rows", "feat"),
        P("rows"),
        P("rows"),
        P(("feat", "rows"), None),
    )
    out_specs = (P("rows"), P(("feat", "rows"), None), P())
    return jax.shard_map(
        on_device, mesh=mesh, in_specs=in_specs, out_specs=out_specs, check_vma=False
    )
```

```python
import jax
import jax.numpy as jnp
from jax import lax
from jax.experimental import pallas as pl
from jax.experimental.pallas import tpu as pltpu
from jax.sharding import PartitionSpec as P

MESH = pl.DeviceIdType.MESH
NZ, NX = 8, 4
N_ROWS = NZ * NX
N_FEAT = 8
BF = jnp.bfloat16
F32 = jnp.float32
I16 = jnp.int16
I32 = jnp.int32
PAIRS = 128
GROUP = 8
VCHUNKS = 8
FSUB = 8


def iota(shape, dim, dtype=I32):
    return lax.broadcasted_iota(I32, shape, dim).astype(dtype)


def body(
    blocks_hbm, counts_hbm, labels_hbm, owner_hbm, w_hbm, values_hbm,
    own_out, grad_out, loss_out,
    blocks_ref, counts_ref, labels_ref, owner_ref, w_ref,
    vbuf, vx, onehot, acc, wtab, cct, qrow, coef, rankhot,
    mbuf, sbuf, rbuf, xrow, gsend, grecv,
    isem, vsem, zs, zr, xs, xr, ms, mr, os_, or_, gs, gr,
):
    r = lax.axis_index("rows")
    f = lax.axis_index("feat")
    z = lax.div(r, NX)
    x = lax.rem(r, NX)

    def row_at(dz, dx):
        return lax.rem(z + dz, NZ) * NX + lax.rem(x + dx, NX)

    def feat_at(df):
        return lax.rem(f + df, N_FEAT)

    def place(dz):
        return ((dz + 2) // 4) % 2, dz // 4, ((dz + 1) // 2) % 2

    fetched = [
        pltpu.make_async_copy(src, dst, isem.at[i])
        for i, (src, dst) in enumerate((
            (w_hbm, w_ref), (blocks_hbm, blocks_ref), (counts_hbm, counts_ref),
            (owner_hbm, owner_ref), (labels_hbm, labels_ref)))
    ]
    for copy in fetched:
        copy.start()

    def vcopy(i):
        n = 2 * PAIRS // VCHUNKS
        part = pl.ds(i * n, n)
        return pltpu.make_async_copy(values_hbm.at[part], vbuf.at[part], vsem.at[i])

    for i in range(VCHUNKS // 2):
        vcopy(i).start()
        vcopy(i + VCHUNKS // 2).start()

    barrier = pltpu.get_barrier_semaphore()
    for dz in (2, 6, 1, 7):
        pl.semaphore_signal(barrier, inc=1, device_id={"rows": row_at(dz, 0)}, device_id_type=MESH)
    for dx in (2, 1, 3):
        pl.semaphore_signal(barrier, inc=1, device_id={"rows": row_at(0, dx)}, device_id_type=MESH)
    for df in range(1, N_FEAT):
        pl.semaphore_signal(barrier, inc=1, device_id={"feat": feat_at(df)}, device_id_type=MESH)

    fetched[0].wait()
    wtab[0, 0, 0, 0] = w_ref[...].astype(BF)
    pl.semaphore_wait(barrier, 4 + NX - 1 + N_FEAT - 1)

    def slot(dz, dx):
        return wtab.at[(*place(dz), dx)]

    def zcopy(dz):
        return pltpu.make_async_remote_copy(
            slot(0, 0), slot(dz, 0), zs, zr.at[dz],
            device_id={"rows": row_at(NZ - dz, 0)}, device_id_type=MESH)

    def xcopy(dz, dx, recv_sem):
        return pltpu.make_async_remote_copy(
            slot(dz, 0), slot(dz, dx), xs, recv_sem,
            device_id={"rows": row_at(0, NX - dx)}, device_id_type=MESH)

    def relay(dz, step, dx):
        return pltpu.make_async_remote_copy(
            slot(dz, 0), slot(dz + step, dx), xs, xr.at[1],
            device_id={"rows": row_at(NZ - step, NX - dx)}, device_id_type=MESH)

    def all_of(ref, send_sem, recv_sem):
        return pltpu.make_async_remote_copy(
            ref, ref, send_sem, recv_sem, device_id={"rows": row_at(0, 1)}, device_id_type=MESH)

    for dz in (2, 6, 1, 7):
        zcopy(dz).start()
    for dx in (2, 1, 3):
        xcopy(0, dx, xr.at[2]).start()

    def pass_on():
        for dz in (1, 7, 2, 6):
            zcopy(dz).wait_recv()
            for dx in (2, 1, 3):
                xcopy(dz, dx, xr.at[place(dz)[0]]).start()
        all_of(gsend.at[0, pl.ds(0, 3)], xs, xr.at[2]).wait_recv()
        for dx in (2, 1, 3, 0):
            relay(2, 2, dx).start()
        for dx in (2, 1, 3, 0):
            relay(2, 1, dx).start()
            relay(6, -1, dx).start()

    fetched[1].wait()
    fetched[2].wait()
    blocks = blocks_ref[...]
    dz = (lax.shift_right_logical(blocks, 7) - z + NZ) & (NZ - 1)
    dx = (lax.shift_right_logical(blocks, 5) - x + NX) & (NX - 1)
    stage = lax.shift_right_logical(dz + 2, 2) & 1
    piece = lax.shift_right_logical(dz + 1, 1) & 1
    code = lax.shift_right_logical(dz, 2) * 512 + stage * 256 + piece * 128 + dx * 32 + (blocks & 31)
    code = jnp.where(iota(blocks.shape, 0) < counts_ref[...], code, -1)
    cct[...] = jnp.concatenate([code[:, :PAIRS], code[:, PAIRS:]], axis=0)

    def build(i, _):
        codes = cct[...]
        for u in range(GROUP):
            k = i * GROUP + u
            wide = jnp.broadcast_to(codes[:, u:u + 1], (PAIRS, PAIRS))
            c16 = wide.astype(I16)
            q16 = (wide & 511).astype(I16)
            rows = pl.ds(pl.multiple_of(k * PAIRS, PAIRS), PAIRS)
            for t in range(4):
                hit = q16 == iota((PAIRS, PAIRS), 1, I16) + jnp.int16(128 * t)
                onehot[t, rows, :] = jnp.where(hit, jnp.ones((), BF), jnp.zeros((), BF))
            v = jnp.concatenate([vbuf[k], vbuf[k + PAIRS]], axis=0)
            zero = jnp.zeros((), BF)
            v1 = jnp.where(c16 >= jnp.int16(512), v, zero)
            vx[0, rows, :] = jnp.where(c16 >= jnp.int16(0), v - v1, zero)
            vx[1, rows, :] = v1
        cct[...] = pltpu.roll(codes, PAIRS - GROUP, 1)
        return 0

    steps = PAIRS // GROUP
    quarter = steps // 4
    for part in range(4):
        vcopy(part).wait()
        vcopy(part + VCHUNKS // 2).wait()
        lax.fori_loop(part * quarter, (part + 1) * quarter, build, 0)
        if part == 1:
            pass_on()
    qrow[...] = (cct[...] & 511).T

    fetched[3].wait()
    fetched[4].wait()
    for h in range(2):
        mine = jnp.broadcast_to(owner_ref[pl.ds(h, 1), :], (PAIRS, PAIRS)).T
        rank = jnp.zeros((PAIRS, 1), F32)
        for g in range(2):
            same = (mine == owner_ref[pl.ds(g, 1), :]) & (
                iota((PAIRS, PAIRS), 1) + g * PAIRS < iota((PAIRS, PAIRS), 0) + h * PAIRS)
            rank = rank + jnp.sum(jnp.where(same, 1.0, 0.0), axis=1, keepdims=True)
        lane = (iota((PAIRS, PAIRS), 1) - 8 * lax.rem(r, 16)).astype(F32)
        rankhot[pl.ds(h * PAIRS, PAIRS), :] = jnp.where(rank == lane, 1.0, 0.0).astype(BF)

    for s in range(2):
        all_of(gsend.at[pl.ds(0, 3), pl.ds(0, 5 if s else 3)], xs, xr.at[s]).wait_recv()
        table = jnp.concatenate([wtab[s, h].reshape(256, 128) for h in range(2)], axis=1)

        def forward(i, _, s=s, table=table):
            for u in range(FSUB):
                k0 = (i * FSUB + u) * GROUP
                rows = pl.ds(pl.multiple_of(k0 * PAIRS, GROUP * PAIRS), GROUP * PAIRS)
                hot = jnp.concatenate([onehot[2 * s, rows, :], onehot[2 * s + 1, rows, :]], axis=1)
                out = jnp.dot(hot, table, preferred_element_type=F32)
                prod = out[:, :128] * vx[0, rows, :].astype(F32) + out[:, 128:] * vx[1, rows, :].astype(F32)
                prod = prod.reshape(GROUP, 2, 8, 8, 128).sum(axis=2)
                for h in range(2):
                    ks = pl.ds(pl.multiple_of(k0 * 8, 8 * GROUP), 8 * GROUP)
                    part = prod[:, h].reshape(8 * GROUP, 128)
                    if s == 0:
                        acc[h, ks, :] = part
                    else:
                        acc[h, ks, :] = acc[h, ks, :] + part
            return 0

        lax.fori_loop(0, steps // FSUB, forward, 0)

    for h in range(2):
        groups = []
        for g in range(PAIRS // 8):
            total = acc[h, pl.ds(64 * g, 8, stride=8), :]
            for i in range(1, 8):
                total = total + acc[h, pl.ds(64 * g + i, 8, stride=8), :]
            groups.append(total)
        rows_sum = jnp.concatenate(groups, axis=0)
        mbuf[f, pl.ds(h, 1), :] = jnp.sum(rows_sum.T, axis=0, keepdims=True)
    for df in (4, 3, 5, 2, 6, 1, 7):
        pltpu.make_async_remote_copy(
            mbuf.at[f], mbuf.at[f], ms, mr,
            device_id={"feat": feat_at(df)}, device_id_type=MESH).start()
    all_of(mbuf.at[pl.ds(0, N_FEAT - 1)], ms, mr).wait_recv()
    margin = mbuf[0]
    for i in range(1, N_FEAT):
        margin = margin + mbuf[i]
    label = labels_ref[...].astype(F32)
    residual = 1.0 / (1.0 + jnp.exp(-margin)) - label
    resid_half = residual.astype(BF).astype(F32)
    spread = [jnp.broadcast_to(resid_half[h:h + 1, :], (PAIRS, PAIRS)).T for h in range(2)]
    coef[...] = jnp.where(iota((PAIRS, PAIRS), 1) < 64, spread[0], spread[1])

    one = jnp.where(r < N_ROWS, 1.0, 0.0)

    def gradient_piece(s, j):
        p = 2 * s + j
        sums = [None, None]
        for t in range(PAIRS // 2):
            left = []
            for u in range(2):
                k = 2 * t + u
                q16 = jnp.broadcast_to(qrow[k:k + 1, :], (16, PAIRS)).astype(I16)
                c16 = jnp.broadcast_to(coef[k:k + 1, :], (16, PAIRS)).astype(BF)
                q16 = jnp.concatenate([q16] * 8, axis=0)
                c16 = jnp.concatenate([c16] * 8, axis=0)
                hit = q16 == iota((128, PAIRS), 0, I16) + jnp.int16(128 * p)
                left.append(jnp.where(hit, c16, jnp.zeros((), BF)))
            rows = pl.ds(t * 2 * PAIRS, 2 * PAIRS)
            right = jnp.concatenate([vx[0, rows, :], vx[1, rows, :]], axis=1)
            d = jnp.dot(jnp.concatenate(left, axis=1), right, preferred_element_type=F32)
            sums[t % 2] = d if sums[t % 2] is None else sums[t % 2] + d
        total = sums[0] + sums[1] * one
        for h in range(2):
            for dx in range(NX):
                block = total[dx * 32:dx * 32 + 32, 128 * h:128 * h + 128]
                if p == 0 and h == 0 and dx == 0:
                    grad_out[...] = block
                else:
                    gsend[p, h * 4 + dx] = block.astype(BF)
        for dz in range(NZ):
            if place(dz)[0] == s and place(dz)[2] == j:
                for dx in (2, 1, 3, 0):
                    if dz != 0 or dx != 0:
                        n = dz // 4 * 4 + dx
                        pltpu.make_async_remote_copy(
                            gsend.at[p, n], grecv.at[p, n], gs.at[p], gr.at[p],
                            device_id={"rows": row_at(dz, dx)}, device_id_type=MESH).start()

    gradient_piece(1, 0)
    gradient_piece(1, 1)

    loss_terms = jnp.maximum(margin, 0.0) + jnp.log1p(jnp.exp(-jnp.abs(margin))) - label * margin
    loss_here = jnp.sum(jnp.sum(loss_terms, axis=1, keepdims=True), axis=0, keepdims=True)
    ordered = jnp.zeros((N_ROWS, 128), F32)
    left = margin
    for _ in range(3):
        piece = left.astype(BF).astype(F32)
        left = left - piece
        pick = jnp.concatenate(
            [jnp.where(owner_ref[pl.ds(h, 1), :] == iota((N_ROWS, 128), 0), piece[h:h + 1, :], 0.0)
             for h in range(2)], axis=1).astype(BF)
        ordered = ordered + jnp.dot(pick, rankhot[...], preferred_element_type=F32)
    lane_group = lax.shift_right_logical(iota((N_ROWS, 128), 1), 3)
    xrow[...] = jnp.where(lane_group == lax.rem(r + 1, 16), loss_here, ordered)
    for d in range(N_ROWS):
        sbuf[d] = xrow[d:d + 1, :]
    rbuf[r] = xrow[pl.ds(r, 1), :]
    for i in range(1, N_ROWS):
        to = row_at(i // NX, i % NX)
        pltpu.make_async_remote_copy(
            sbuf.at[to], rbuf.at[r], os_, or_,
            device_id={"rows": to}, device_id_type=MESH).start()

    gradient_piece(0, 1)
    gradient_piece(0, 0)

    all_of(rbuf.at[pl.ds(0, N_ROWS - 1)], os_, or_).wait_recv()
    group1 = lax.shift_right_logical(iota((1, 128), 1), 3)
    loss_sum = jnp.zeros((1, 128), F32)
    for h in range(2):
        mine = jnp.zeros((1, 128), F32)
        for g in range(16):
            row = rbuf[h * 16 + g]
            mine = mine + jnp.where(group1 == g, row, 0.0)
            loss_sum = loss_sum + jnp.where(group1 == (g + 1) % 16, row, 0.0)
        own_out[pl.ds(h, 1), :] = mine
    loss_total = jnp.sum(loss_sum, axis=1, keepdims=True) * (1.0 / (8.0 * 8192.0))
    loss_out[...] = jnp.broadcast_to(loss_total, (1, 128))

    total = grad_out[...]
    for p in (2, 3, 1, 0):
        first = 0 if p else 1
        all_of(grecv.at[p, pl.ds(first, 8 - first)], gs.at[p], gr.at[p]).wait_recv()
        for n in range(first, 8):
            total = total + grecv[p, n].astype(F32)
    grad_out[...] = total

    all_of(gsend.at[0, pl.ds(0, 4)], zs, zr.at[0]).wait_send()
    all_of(vx.at[0, pl.ds(0, 27 * 32)], xs, xr.at[0]).wait_send()
    all_of(mbuf.at[pl.ds(0, N_FEAT - 1)], ms, mr).wait_send()
    all_of(sbuf.at[pl.ds(0, N_ROWS - 1)], os_, or_).wait_send()
    for p in range(4):
        first = 0 if p else 1
        all_of(gsend.at[p, pl.ds(first, 8 - first)], gs.at[p], gr.at[p]).wait_send()


def finish(own_in, grad_in, loss_in, own_out, grad_out, loss_out):
    own_out[...] = own_in[...]
    grad_out[...] = grad_in[...]
    loss_out[...] = loss_in[...]


def on_device(tile_values, tile_blocks, tile_counts, labels, owner_rank, weights):
    vmem = pl.BlockSpec(memory_space=pltpu.VMEM)
    dma = pltpu.SemaphoreType.DMA
    results = (
        jax.ShapeDtypeStruct((2, 128), F32),
        jax.ShapeDtypeStruct((32, 128), F32),
        jax.ShapeDtypeStruct((1, 128), F32),
    )
    parts = pl.pallas_call(
        body,
        out_shape=results,
        in_specs=[pl.BlockSpec(memory_space=pl.ANY)] * 6,
        out_specs=(vmem, vmem, vmem),
        scratch_shapes=[
            pltpu.VMEM((64, 256), I32),
            pltpu.VMEM((1, 256), I32),
            pltpu.VMEM((2, 128), I32),
            pltpu.VMEM((2, 128), I32),
            pltpu.VMEM((32, 128), F32),
            pltpu.VMEM((256, 64, 128), BF),
            pltpu.VMEM((2, 16384, 128), BF),
            pltpu.VMEM((4, 16384, 128), BF),
            pltpu.VMEM((2, PAIRS * 8, 128), F32),
            pltpu.VMEM((2, 2, 2, NX, 32, 128), BF),
            pltpu.VMEM((PAIRS, PAIRS), I32),
            pltpu.VMEM((PAIRS, PAIRS), I32),
            pltpu.VMEM((PAIRS, PAIRS), F32),
            pltpu.VMEM((256, 128), BF),
            pltpu.VMEM((N_FEAT, 2, 128), F32),
            pltpu.VMEM((N_ROWS, 1, 128), F32),
            pltpu.VMEM((N_ROWS, 1, 128), F32),
            pltpu.VMEM((N_ROWS, 128), F32),
            pltpu.VMEM((4, 8, 32, 128), BF),
            pltpu.VMEM((4, 8, 32, 128), BF),
            dma((5,)), dma((VCHUNKS,)),
            dma, dma((NZ,)),
            dma, dma((3,)),
            dma, dma,
            dma, dma,
            dma((4,)), dma((4,)),
        ],
        compiler_params=pltpu.CompilerParams(
            collective_id=0, has_side_effects=True, vmem_limit_bytes=56 * 1024 * 1024),
    )(tile_blocks.T, tile_counts.T, labels.reshape(2, 128), owner_rank.reshape(2, 128), weights, tile_values)
    own, grad, loss = pl.pallas_call(
        finish, out_shape=results, in_specs=[vmem] * 3, out_specs=(vmem, vmem, vmem),
    )(*parts)
    return own.reshape(256), grad, loss[0, 0]


def solution(mesh):
    in_specs = (
        P("rows", "feat", None),
        P("rows", "feat"),
        P("rows", "feat"),
        P("rows"),
        P("rows"),
        P(("feat", "rows"), None),
    )
    out_specs = (P("rows"), P(("feat", "rows"), None), P())
    return jax.shard_map(
        on_device, mesh=mesh, in_specs=in_specs, out_specs=out_specs, check_vma=False
    )
```

```python
import jax
import jax.numpy as jnp
from jax import lax
from jax.experimental import pallas as pl
from jax.experimental.pallas import tpu as pltpu
from jax.sharding import PartitionSpec as P

MESH = pl.DeviceIdType.MESH
NZ, NX = 8, 4
N_ROWS = NZ * NX
N_FEAT = 8
BF = jnp.bfloat16
F32 = jnp.float32
I16 = jnp.int16
I32 = jnp.int32
PAIRS = 128
GROUP = 8
VCHUNKS = 8
LAG = 6
ZTILE = 40
SUMMED = (2, 3)


def iota(shape, dim, dtype=I32):
    return lax.broadcasted_iota(I32, shape, dim).astype(dtype)


def body(
    blocks_hbm, counts_hbm, labels_hbm, owner_hbm, w_hbm, values_hbm,
    own_out, grad_out, loss_out,
    blocks_ref, counts_ref, labels_ref, owner_ref, w_ref,
    vbuf, vx, onehot, acc, wtab, cct, qrow, coef, rankhot,
    mbuf, sbuf, rbuf, xrow, kept, gsend, grecv,
    isem, vsem, zs, zr, xs, xr, ms, mr, os_, or_, gs, gr, fs, fr,
):
    r = lax.axis_index("rows")
    f = lax.axis_index("feat")
    z = lax.div(r, NX)
    x = lax.rem(r, NX)

    def row_at(dz, dx):
        return lax.rem(z + dz, NZ) * NX + lax.rem(x + dx, NX)

    def feat_at(df):
        return lax.rem(f + df, N_FEAT)

    def place(dz, dx):
        dz, dx = {(7, 2): (1, 0), (1, 0): (7, 2)}.get((dz, dx), (dz, dx))
        return ((dz + 2) // 4) % 2, dz // 4, ((dz + 1) // 2) % 2, dx

    fetched = [
        pltpu.make_async_copy(src, dst, isem.at[i])
        for i, (src, dst) in enumerate((
            (w_hbm, w_ref), (blocks_hbm, blocks_ref), (counts_hbm, counts_ref),
            (owner_hbm, owner_ref), (labels_hbm, labels_ref)))
    ]
    for copy in fetched:
        copy.start()

    def vcopy(i):
        n = 2 * PAIRS // VCHUNKS
        part = pl.ds(i * n, n)
        return pltpu.make_async_copy(values_hbm.at[part], vbuf.at[part], vsem.at[i])

    for i in range(VCHUNKS // 2):
        vcopy(i).start()
        vcopy(i + VCHUNKS // 2).start()

    barrier = pltpu.get_barrier_semaphore()
    for dz in (2, 6, 1, 7):
        pl.semaphore_signal(barrier, inc=1, device_id={"rows": row_at(dz, 0)}, device_id_type=MESH)
    for dx in (2, 1, 3):
        pl.semaphore_signal(barrier, inc=1, device_id={"rows": row_at(0, dx)}, device_id_type=MESH)
    for df in range(1, N_FEAT):
        pl.semaphore_signal(barrier, inc=1, device_id={"feat": feat_at(df)}, device_id_type=MESH)

    fetched[0].wait()
    wtab[0, 0, 0, 0] = w_ref[...].astype(BF)
    pl.semaphore_wait(barrier, 4 + NX - 1 + N_FEAT - 1)

    def slot(dz, dx):
        return wtab.at[place(dz, dx)]

    def zcopy(dz):
        return pltpu.make_async_remote_copy(
            slot(0, 0), slot(dz, 0), zs, zr.at[dz],
            device_id={"rows": row_at(NZ - dz, 0)}, device_id_type=MESH)

    def xcopy(dz, dx, recv_sem):
        return pltpu.make_async_remote_copy(
            slot(dz, 0), slot(dz, dx), xs, recv_sem,
            device_id={"rows": row_at(0, NX - dx)}, device_id_type=MESH)

    def relay(dz, step, dx):
        return pltpu.make_async_remote_copy(
            slot(dz, 0), slot(dz + step, dx), xs, xr.at[1],
            device_id={"rows": row_at(NZ - step, NX - dx)}, device_id_type=MESH)

    def all_of(ref, send_sem, recv_sem):
        return pltpu.make_async_remote_copy(
            ref, ref, send_sem, recv_sem, device_id={"rows": row_at(0, 1)}, device_id_type=MESH)

    for dz in (2, 6, 1, 7):
        zcopy(dz).start()
    for dx in (2, 1, 3):
        xcopy(0, dx, xr.at[2]).start()

    def pass_on(*arrivals):
        for dz in arrivals:
            zcopy(dz).wait_recv()
            for dx in (2, 1, 3):
                xcopy(dz, dx, xr.at[place(dz, dx)[0]]).start()

    def pass_far():
        pass_on(2)
        all_of(vx.at[0, pl.ds(0, 3 * 32)], xs, xr.at[2]).wait_recv()
        for dx in (2, 1, 3, 0):
            relay(2, 2, dx).start()
        for dx in (2, 1, 3, 0):
            relay(2, 1, dx).start()
            relay(6, -1, dx).start()

    fetched[1].wait()
    fetched[2].wait()
    blocks = blocks_ref[...]
    dz = (lax.shift_right_logical(blocks, 7) - z + NZ) & (NZ - 1)
    dx = (lax.shift_right_logical(blocks, 5) - x + NX) & (NX - 1)
    peer = dz * NX + dx
    peer = jnp.where(peer == 7 * NX + 2, NX, jnp.where(peer == NX, 7 * NX + 2, peer))
    dz = lax.shift_right_logical(peer, 2)
    dx = peer & (NX - 1)
    stage = lax.shift_right_logical(dz + 2, 2) & 1
    piece = lax.shift_right_logical(dz + 1, 1) & 1
    code = lax.shift_right_logical(dz, 2) * 512 + stage * 256 + piece * 128 + dx * 32 + (blocks & 31)
    code = jnp.where(iota(blocks.shape, 0) < counts_ref[...], code, -1)
    cct[...] = jnp.concatenate([code[:, :PAIRS], code[:, PAIRS:]], axis=0)

    def build(i, _):
        codes = cct[...]
        for u in range(GROUP):
            k = i * GROUP + u
            wide = jnp.broadcast_to(codes[:, u:u + 1], (PAIRS, PAIRS))
            c16 = wide.astype(I16)
            q16 = (wide & 511).astype(I16)
            rows = pl.ds(pl.multiple_of(k * PAIRS, PAIRS), PAIRS)
            for t in range(4):
                hit = q16 == iota((PAIRS, PAIRS), 1, I16) + jnp.int16(128 * t)
                onehot[t, rows, :] = jnp.where(hit, jnp.ones((), BF), jnp.zeros((), BF))
            v = jnp.concatenate([vbuf[k], vbuf[k + PAIRS]], axis=0)
            zero = jnp.zeros((), BF)
            v1 = jnp.where(c16 >= jnp.int16(512), v, zero)
            vx[0, rows, :] = jnp.where(c16 >= jnp.int16(0), v - v1, zero)
            vx[1, rows, :] = v1
        cct[...] = pltpu.roll(codes, PAIRS - GROUP, 1)
        return 0

    steps = PAIRS // GROUP
    quarter = steps // 4
    for part in range(4):
        vcopy(part).wait()
        vcopy(part + VCHUNKS // 2).wait()
        lax.fori_loop(part * quarter, (part + 1) * quarter, build, 0)
        if part == 1:
            pass_on(1, 7, 6)
            pass_far()
    qrow[...] = (cct[...] & 511).T

    fetched[3].wait()
    fetched[4].wait()
    for h in range(2):
        mine = jnp.broadcast_to(owner_ref[pl.ds(h, 1), :], (PAIRS, PAIRS)).T
        rank = jnp.zeros((PAIRS, 1), F32)
        for g in range(2):
            same = (mine == owner_ref[pl.ds(g, 1), :]) & (
                iota((PAIRS, PAIRS), 1) + g * PAIRS < iota((PAIRS, PAIRS), 0) + h * PAIRS)
            rank = rank + jnp.sum(jnp.where(same, 1.0, 0.0), axis=1, keepdims=True)
        lane = (iota((PAIRS, PAIRS), 1) - 8 * lax.rem(r, 16)).astype(F32)
        rankhot[pl.ds(h * PAIRS, PAIRS), :] = jnp.where(rank == lane, 1.0, 0.0).astype(BF)

    for s in range(2):
        all_of(vx.at[0, pl.ds(0, (15 if s else 9) * 32)], xs, xr.at[s]).wait_recv()
        table = jnp.concatenate([wtab[s, h].reshape(256, 128) for h in range(2)], axis=1)

        for u in range(steps):
            k0 = u * GROUP
            rows = pl.ds(k0 * PAIRS, GROUP * PAIRS)
            hot = jnp.concatenate([onehot[2 * s, rows, :], onehot[2 * s + 1, rows, :]], axis=1)
            out = jnp.dot(hot, table, preferred_element_type=F32)
            prod = out[:, :128] * vx[0, rows, :].astype(F32) + out[:, 128:] * vx[1, rows, :].astype(F32)
            prod = prod.reshape(GROUP, 2, 8, 8, 128).sum(axis=2)
            for h in range(2):
                ks = pl.ds(k0 * 8, 8 * GROUP)
                part = prod[:, h].reshape(8 * GROUP, 128)
                if s == 0:
                    acc[h, ks, :] = part
                else:
                    acc[h, ks, :] = acc[h, ks, :] + part

    for h in range(2):
        groups = []
        for g in range(PAIRS // 8):
            total = acc[h, pl.ds(64 * g, 8, stride=8), :]
            for i in range(1, 8):
                total = total + acc[h, pl.ds(64 * g + i, 8, stride=8), :]
            groups.append(total)
        rows_sum = jnp.concatenate(groups, axis=0)
        mbuf[f, pl.ds(h, 1), :] = jnp.sum(rows_sum.T, axis=0, keepdims=True)
    for df in (4, 3, 5, 2, 6, 1, 7):
        pltpu.make_async_remote_copy(
            mbuf.at[f], mbuf.at[f], ms, mr,
            device_id={"feat": feat_at(df)}, device_id_type=MESH).start()
    all_of(mbuf.at[pl.ds(0, N_FEAT - 1)], ms, mr).wait_recv()
    margin = mbuf[0]
    for i in range(1, N_FEAT):
        margin = margin + mbuf[i]
    label = labels_ref[...].astype(F32)
    residual = 1.0 / (1.0 + jnp.exp(-margin)) - label
    resid_half = residual.astype(BF).astype(F32)
    spread = [jnp.broadcast_to(resid_half[h:h + 1, :], (PAIRS, PAIRS)).T for h in range(2)]
    coef[...] = jnp.where(iota((PAIRS, PAIRS), 1) < 64, spread[0], spread[1])

    loss_terms = jnp.maximum(margin, 0.0) + jnp.log1p(jnp.exp(-jnp.abs(margin))) - label * margin
    loss_here = jnp.sum(jnp.sum(loss_terms, axis=1, keepdims=True), axis=0, keepdims=True)
    ordered = jnp.zeros((N_ROWS, 128), F32)
    left = margin
    for _ in range(3):
        piece = left.astype(BF).astype(F32)
        left = left - piece
        pick = jnp.concatenate(
            [jnp.where(owner_ref[pl.ds(h, 1), :] == iota((N_ROWS, 128), 0), piece[h:h + 1, :], 0.0)
             for h in range(2)], axis=1).astype(BF)
        ordered = ordered + jnp.dot(pick, rankhot[...], preferred_element_type=F32)
    lane_group = lax.shift_right_logical(iota((N_ROWS, 128), 1), 3)
    xrow[...] = jnp.where(lane_group == lax.rem(r + 1, 16), loss_here, ordered)
    for d in range(N_ROWS):
        sbuf[d] = xrow[d:d + 1, :]
    rbuf[r] = xrow[pl.ds(r, 1), :]
    def send_rows():
        for i in range(1, N_ROWS):
            to = row_at(i // NX, i % NX)
            pltpu.make_async_remote_copy(
                sbuf.at[to], rbuf.at[r], os_, or_,
                device_id={"rows": to}, device_id_type=MESH).start()

    one = jnp.where(r < N_ROWS, 1.0, 0.0)
    sums = {p: [None, None] for p in range(4)}

    def tiles(p, first, last):
        for t in range(first, last):
            left = []
            for u in range(2):
                k = 2 * t + u
                q16 = jnp.broadcast_to(qrow[k:k + 1, :], (16, PAIRS)).astype(I16)
                c16 = jnp.broadcast_to(coef[k:k + 1, :], (16, PAIRS)).astype(BF)
                q16 = jnp.concatenate([q16] * 8, axis=0)
                c16 = jnp.concatenate([c16] * 8, axis=0)
                hit = q16 == iota((128, PAIRS), 0, I16) + jnp.int16(128 * p)
                left.append(jnp.where(hit, c16, jnp.zeros((), BF)))
            rows = pl.ds(t * 2 * PAIRS, 2 * PAIRS)
            right = jnp.concatenate([vx[0, rows, :], vx[1, rows, :]], axis=1)
            d = jnp.dot(jnp.concatenate(left, axis=1), right, preferred_element_type=F32)
            sums[p][t % 2] = d if sums[p][t % 2] is None else sums[p][t % 2] + d

    def send_piece(p):
        total = sums[p][0] + sums[p][1] * one
        for h in range(2):
            for c in range(NX):
                block = total[c * 32:c * 32 + 32, 128 * h:128 * h + 128]
                if c == 0 and (p in SUMMED or p == 0 and h == 0):
                    kept[p, h] = block
                else:
                    gsend[p, c, h] = block.astype(BF)
        if p in SUMMED:
            for dx in (2, 1, 3):
                pltpu.make_async_remote_copy(
                    gsend.at[p, dx], grecv.at[p, dx], gs.at[p], gr.at[p],
                    device_id={"rows": row_at(0, dx)}, device_id_type=MESH).start()
            return
        for dx in (2, 1, 3, 0):
            for dz in (4, 3, 5, 2, 6, 1, 7, 0):
                s, h, j, c = place(dz, dx)
                if 2 * s + j == p and (dz != 0 or dx != 0):
                    pltpu.make_async_remote_copy(
                        gsend.at[p, c, h], grecv.at[p, c, h], gs.at[p], gr.at[p],
                        device_id={"rows": row_at(dz, dx)}, device_id_type=MESH).start()

    def along_z(p):
        all_of(gsend.at[p, pl.ds(1, NX - 1)], gs.at[p], gr.at[p]).wait_recv()
        for h in range(2):
            block = kept[p, h]
            for dx in range(1, NX):
                block = block + grecv[p, dx, h].astype(F32)
            gsend[p, 0, h] = block.astype(BF)
        for dz in (4, 3, 5, 2):
            s, h, j, _ = place(dz, 0)
            if 2 * s + j == p:
                pltpu.make_async_remote_copy(
                    gsend.at[p, 0, h], grecv.at[p, 0, h], fs, fr,
                    device_id={"rows": row_at(dz, 0)}, device_id_type=MESH).start()

    count = PAIRS // 2
    tiles(2, 0, count)
    tiles(3, 0, LAG)
    send_piece(2)
    tiles(3, LAG, count)
    tiles(1, 0, LAG)
    send_piece(3)
    send_rows()
    tiles(1, LAG, count)
    tiles(0, 0, LAG)
    send_piece(1)
    tiles(0, LAG, ZTILE)
    along_z(2)
    tiles(0, ZTILE, count)
    send_piece(0)
    if 3 in SUMMED:
        along_z(3)

    all_of(rbuf.at[pl.ds(0, N_ROWS - 1)], os_, or_).wait_recv()
    group1 = lax.shift_right_logical(iota((1, 128), 1), 3)
    loss_sum = jnp.zeros((1, 128), F32)
    for h in range(2):
        mine = jnp.zeros((1, 128), F32)
        for g in range(16):
            row = rbuf[h * 16 + g]
            mine = mine + jnp.where(group1 == g, row, 0.0)
            loss_sum = loss_sum + jnp.where(group1 == (g + 1) % 16, row, 0.0)
        own_out[pl.ds(h, 1), :] = mine
    loss_total = jnp.sum(loss_sum, axis=1, keepdims=True) * (1.0 / (8.0 * 8192.0))
    loss_out[...] = jnp.broadcast_to(loss_total, (1, 128))

    total = kept[0, 0]
    for p in (3, 1, 2, 0):
        if p in SUMMED:
            continue
        first = 0 if p else 1
        all_of(vx.at[0, pl.ds(0, (8 - first) * 32)], gs.at[p], gr.at[p]).wait_recv()
        for n in range(first, 8):
            total = total + grecv[p, n // 2, n % 2].astype(F32)
    all_of(vx.at[0, pl.ds(0, 2 * len(SUMMED) * 32)], fs, fr).wait_recv()
    for p in SUMMED:
        for h in range(2):
            total = total + grecv[p, 0, h].astype(F32)
    grad_out[...] = total

    all_of(vx.at[0, pl.ds(0, 4 * 32)], zs, zr.at[0]).wait_send()
    all_of(vx.at[0, pl.ds(0, 27 * 32)], xs, xr.at[0]).wait_send()
    all_of(mbuf.at[pl.ds(0, N_FEAT - 1)], ms, mr).wait_send()
    all_of(sbuf.at[pl.ds(0, N_ROWS - 1)], os_, or_).wait_send()
    for p in range(4):
        sent = 6 if p in SUMMED else 8 if p else 7
        all_of(vx.at[0, pl.ds(0, sent * 32)], gs.at[p], gr.at[p]).wait_send()
    all_of(vx.at[0, pl.ds(0, 2 * len(SUMMED) * 32)], fs, fr).wait_send()


def finish(own_in, grad_in, loss_in, own_out, grad_out, loss_out):
    own_out[...] = own_in[...]
    grad_out[...] = grad_in[...]
    loss_out[...] = loss_in[...]


def on_device(tile_values, tile_blocks, tile_counts, labels, owner_rank, weights):
    vmem = pl.BlockSpec(memory_space=pltpu.VMEM)
    dma = pltpu.SemaphoreType.DMA
    results = (
        jax.ShapeDtypeStruct((2, 128), F32),
        jax.ShapeDtypeStruct((32, 128), F32),
        jax.ShapeDtypeStruct((1, 128), F32),
    )
    parts = pl.pallas_call(
        body,
        out_shape=results,
        in_specs=[pl.BlockSpec(memory_space=pl.ANY)] * 6,
        out_specs=(vmem, vmem, vmem),
        scratch_shapes=[
            pltpu.VMEM((64, 256), I32),
            pltpu.VMEM((1, 256), I32),
            pltpu.VMEM((2, 128), I32),
            pltpu.VMEM((2, 128), I32),
            pltpu.VMEM((32, 128), F32),
            pltpu.VMEM((256, 64, 128), BF),
            pltpu.VMEM((2, 16384, 128), BF),
            pltpu.VMEM((4, 16384, 128), BF),
            pltpu.VMEM((2, PAIRS * 8, 128), F32),
            pltpu.VMEM((2, 2, 2, NX, 32, 128), BF),
            pltpu.VMEM((PAIRS, PAIRS), I32),
            pltpu.VMEM((PAIRS, PAIRS), I32),
            pltpu.VMEM((PAIRS, PAIRS), F32),
            pltpu.VMEM((256, 128), BF),
            pltpu.VMEM((N_FEAT, 2, 128), F32),
            pltpu.VMEM((N_ROWS, 1, 128), F32),
            pltpu.VMEM((N_ROWS, 1, 128), F32),
            pltpu.VMEM((N_ROWS, 128), F32),
            pltpu.VMEM((4, 2, 32, 128), F32),
            pltpu.VMEM((4, NX, 2, 32, 128), BF),
            pltpu.VMEM((4, NX, 2, 32, 128), BF),
            dma((5,)), dma((VCHUNKS,)),
            dma, dma((NZ,)),
            dma, dma((3,)),
            dma, dma,
            dma, dma,
            dma((4,)), dma((4,)),
            dma, dma,
        ],
        compiler_params=pltpu.CompilerParams(
            collective_id=0, has_side_effects=True, vmem_limit_bytes=40 * 1024 * 1024),
    )(*[pltpu.with_memory_space_constraint(a, pltpu.HBM) for a in (tile_blocks.T, tile_counts.T, labels.reshape(2, 128), owner_rank.reshape(2, 128), weights, tile_values)])
    own, grad, loss = pl.pallas_call(
        finish, out_shape=results, in_specs=[vmem] * 3, out_specs=(vmem, vmem, vmem),
        compiler_params=pltpu.CompilerParams(vmem_limit_bytes=1024 * 1024),
    )(*parts)
    return own.reshape(256), grad, loss[0, 0]


def solution(mesh):
    in_specs = (
        P("rows", "feat", None),
        P("rows", "feat"),
        P("rows", "feat"),
        P("rows"),
        P("rows"),
        P(("feat", "rows"), None),
    )
    out_specs = (P("rows"), P(("feat", "rows"), None), P())
    return jax.shard_map(
        on_device, mesh=mesh, in_specs=in_specs, out_specs=out_specs, check_vma=False
    )
```

```python
import jax
import jax.numpy as jnp
from jax import lax
from jax.experimental import pallas as pl
from jax.experimental.pallas import tpu as pltpu
from jax.sharding import PartitionSpec as P

MESH = pl.DeviceIdType.MESH
NZ, NX = 8, 4
N_ROWS = NZ * NX
N_FEAT = 8
BF = jnp.bfloat16
F32 = jnp.float32
I16 = jnp.int16
I32 = jnp.int32
PAIRS = 128
GROUP = 8
VCHUNKS = 8
LAG = 6
ZTILE = 40
SUMMED = (2, 3)


def iota(shape, dim, dtype=I32):
    return lax.broadcasted_iota(I32, shape, dim).astype(dtype)


def body(
    blocks_hbm, counts_hbm, labels_hbm, owner_hbm, w_hbm, values_hbm,
    own_out, grad_out, loss_out,
    blocks_ref, counts_ref, labels_ref, owner_ref, w_ref,
    vbuf, vx, onehot, acc, wtab, cct, qrow, coef, rankhot,
    mbuf, sbuf, rbuf, xrow, kept, gsend, grecv,
    isem, vsem, zs, zr, xs, xr, ms, mr, os_, or_, gs, gr, fs, fr,
):
    r = lax.axis_index("rows")
    f = lax.axis_index("feat")
    z = lax.div(r, NX)
    x = lax.rem(r, NX)

    def row_at(dz, dx):
        return lax.rem(z + dz, NZ) * NX + lax.rem(x + dx, NX)

    def feat_at(df):
        return lax.rem(f + df, N_FEAT)

    def place(dz, dx):
        dz, dx = {(7, 2): (1, 0), (1, 0): (7, 2)}.get((dz, dx), (dz, dx))
        return ((dz + 2) // 4) % 2, dz // 4, ((dz + 1) // 2) % 2, dx

    fetched = [
        pltpu.make_async_copy(src, dst, isem.at[i])
        for i, (src, dst) in enumerate((
            (w_hbm, w_ref), (blocks_hbm, blocks_ref), (counts_hbm, counts_ref),
            (owner_hbm, owner_ref), (labels_hbm, labels_ref)))
    ]
    for copy in fetched:
        copy.start()

    def vcopy(i):
        n = 2 * PAIRS // VCHUNKS
        part = pl.ds(i * n, n)
        return pltpu.make_async_copy(values_hbm.at[part], vbuf.at[part], vsem.at[i])

    for i in range(VCHUNKS // 2):
        vcopy(i).start()
        vcopy(i + VCHUNKS // 2).start()

    barrier = pltpu.get_barrier_semaphore()
    for dz in (2, 6, 1, 7):
        pl.semaphore_signal(barrier, inc=1, device_id={"rows": row_at(dz, 0)}, device_id_type=MESH)
    for dx in (2, 1, 3):
        pl.semaphore_signal(barrier, inc=1, device_id={"rows": row_at(0, dx)}, device_id_type=MESH)
    for df in range(1, N_FEAT):
        pl.semaphore_signal(barrier, inc=1, device_id={"feat": feat_at(df)}, device_id_type=MESH)

    fetched[0].wait()
    wtab[0, 0, 0, 0] = w_ref[...].astype(BF)
    pl.semaphore_wait(barrier, 4 + NX - 1 + N_FEAT - 1)

    def slot(dz, dx):
        return wtab.at[place(dz, dx)]

    def zcopy(dz):
        return pltpu.make_async_remote_copy(
            slot(0, 0), slot(dz, 0), zs, zr.at[dz],
            device_id={"rows": row_at(NZ - dz, 0)}, device_id_type=MESH)

    def xcopy(dz, dx, recv_sem):
        return pltpu.make_async_remote_copy(
            slot(dz, 0), slot(dz, dx), xs, recv_sem,
            device_id={"rows": row_at(0, NX - dx)}, device_id_type=MESH)

    def relay(dz, step, dx):
        return pltpu.make_async_remote_copy(
            slot(dz, 0), slot(dz + step, dx), xs, xr.at[1],
            device_id={"rows": row_at(NZ - step, NX - dx)}, device_id_type=MESH)

    def all_of(ref, send_sem, recv_sem):
        return pltpu.make_async_remote_copy(
            ref, ref, send_sem, recv_sem, device_id={"rows": row_at(0, 1)}, device_id_type=MESH)

    for dz in (2, 6, 1, 7):
        zcopy(dz).start()
    for dx in (2, 1, 3):
        xcopy(0, dx, xr.at[2]).start()

    def pass_on(*arrivals):
        for dz in arrivals:
            zcopy(dz).wait_recv()
            for dx in (2, 1, 3):
                xcopy(dz, dx, xr.at[place(dz, dx)[0]]).start()

    def pass_far():
        pass_on(2)
        all_of(vx.at[pl.ds(0, 3 * 16)], xs, xr.at[2]).wait_recv()
        for dx in (2, 1, 3, 0):
            relay(2, 2, dx).start()
        for dx in (2, 1, 3, 0):
            relay(2, 1, dx).start()
            relay(6, -1, dx).start()

    fetched[1].wait()
    fetched[2].wait()
    blocks = blocks_ref[...]
    dz = (lax.shift_right_logical(blocks, 7) - z + NZ) & (NZ - 1)
    dx = (lax.shift_right_logical(blocks, 5) - x + NX) & (NX - 1)
    peer = dz * NX + dx
    peer = jnp.where(peer == 7 * NX + 2, NX, jnp.where(peer == NX, 7 * NX + 2, peer))
    dz = lax.shift_right_logical(peer, 2)
    dx = peer & (NX - 1)
    stage = lax.shift_right_logical(dz + 2, 2) & 1
    piece = lax.shift_right_logical(dz + 1, 1) & 1
    code = lax.shift_right_logical(dz, 2) * 512 + stage * 256 + piece * 128 + dx * 32 + (blocks & 31)
    code = jnp.where(iota(blocks.shape, 0) < counts_ref[...], code, -1)
    cct[...] = jnp.concatenate([code[:, :PAIRS], code[:, PAIRS:]], axis=0)

    def build(i, _):
        codes = cct[...]
        for u in range(GROUP):
            k = i * GROUP + u
            wide = jnp.broadcast_to(codes[:, u:u + 1], (PAIRS, PAIRS))
            c16 = wide.astype(I16)
            q16 = (wide & 511).astype(I16)
            rows = pl.ds(pl.multiple_of(k * PAIRS, PAIRS), PAIRS)
            for s in range(2):
                hits = [q16 == iota((PAIRS, PAIRS), 1, I16) + jnp.int16(256 * s + 128 * t) for t in range(2)]
                onehot[s, rows, :] = jnp.concatenate(
                    [jnp.where(hit, jnp.ones((), BF), jnp.zeros((), BF)) for hit in hits], axis=1)
            v = jnp.concatenate([vbuf[k], vbuf[k + PAIRS]], axis=0)
            zero = jnp.zeros((), BF)
            v1 = jnp.where(c16 >= jnp.int16(512), v, zero)
            vx[rows, :] = jnp.concatenate([jnp.where(c16 >= jnp.int16(0), v - v1, zero), v1], axis=1)
        cct[...] = pltpu.roll(codes, PAIRS - GROUP, 1)
        return 0

    steps = PAIRS // GROUP
    quarter = steps // 4
    for part in range(4):
        vcopy(part).wait()
        vcopy(part + VCHUNKS // 2).wait()
        lax.fori_loop(part * quarter, (part + 1) * quarter, build, 0)
        if part == 1:
            pass_on(1, 7, 6)
            pass_far()
    qrow[...] = (cct[...] & 511).T

    fetched[3].wait()
    fetched[4].wait()
    for h in range(2):
        mine = jnp.broadcast_to(owner_ref[pl.ds(h, 1), :], (PAIRS, PAIRS)).T
        rank = jnp.zeros((PAIRS, 1), F32)
        for g in range(2):
            same = (mine == owner_ref[pl.ds(g, 1), :]) & (
                iota((PAIRS, PAIRS), 1) + g * PAIRS < iota((PAIRS, PAIRS), 0) + h * PAIRS)
            rank = rank + jnp.sum(jnp.where(same, 1.0, 0.0), axis=1, keepdims=True)
        lane = (iota((PAIRS, PAIRS), 1) - 8 * lax.rem(r, 16)).astype(F32)
        rankhot[pl.ds(h * PAIRS, PAIRS), :] = jnp.where(rank == lane, 1.0, 0.0).astype(BF)

    for s in range(2):
        all_of(vx.at[pl.ds(0, (15 if s else 9) * 16)], xs, xr.at[s]).wait_recv()
        table = jnp.concatenate([wtab[s, h].reshape(256, 128) for h in range(2)], axis=1)

        for u in range(steps):
            k0 = u * GROUP
            rows = pl.ds(k0 * PAIRS, GROUP * PAIRS)
            out = jnp.dot(onehot[s, rows, :], table, preferred_element_type=F32)
            prod = out * vx[rows, :].astype(F32)
            prod = prod[:, :128] + prod[:, 128:]
            prod = prod.reshape(GROUP, 2, 8, 8, 128).sum(axis=2)
            for h in range(2):
                ks = pl.ds(k0 * 8, 8 * GROUP)
                part = prod[:, h].reshape(8 * GROUP, 128)
                if s == 0:
                    acc[h, ks, :] = part
                else:
                    acc[h, ks, :] = acc[h, ks, :] + part

    for h in range(2):
        groups = []
        for g in range(PAIRS // 8):
            total = acc[h, pl.ds(64 * g, 8, stride=8), :]
            for i in range(1, 8):
                total = total + acc[h, pl.ds(64 * g + i, 8, stride=8), :]
            groups.append(total)
        rows_sum = jnp.concatenate(groups, axis=0)
        mbuf[f, pl.ds(h, 1), :] = jnp.sum(rows_sum.T, axis=0, keepdims=True)
    for df in (4, 3, 5, 2, 6, 1, 7):
        pltpu.make_async_remote_copy(
            mbuf.at[f], mbuf.at[f], ms, mr,
            device_id={"feat": feat_at(df)}, device_id_type=MESH).start()
    all_of(mbuf.at[pl.ds(0, N_FEAT - 1)], ms, mr).wait_recv()
    margin = mbuf[0]
    for i in range(1, N_FEAT):
        margin = margin + mbuf[i]
    label = labels_ref[...].astype(F32)
    residual = 1.0 / (1.0 + jnp.exp(-margin)) - label
    resid_half = residual.astype(BF).astype(F32)
    spread = [jnp.broadcast_to(resid_half[h:h + 1, :], (PAIRS, PAIRS)).T for h in range(2)]
    coef[...] = jnp.where(iota((PAIRS, PAIRS), 1) < 64, spread[0], spread[1])

    loss_terms = jnp.maximum(margin, 0.0) + jnp.log1p(jnp.exp(-jnp.abs(margin))) - label * margin
    loss_here = jnp.sum(jnp.sum(loss_terms, axis=1, keepdims=True), axis=0, keepdims=True)
    ordered = jnp.zeros((N_ROWS, 128), F32)
    left = margin
    for _ in range(3):
        piece = left.astype(BF).astype(F32)
        left = left - piece
        pick = jnp.concatenate(
            [jnp.where(owner_ref[pl.ds(h, 1), :] == iota((N_ROWS, 128), 0), piece[h:h + 1, :], 0.0)
             for h in range(2)], axis=1).astype(BF)
        ordered = ordered + jnp.dot(pick, rankhot[...], preferred_element_type=F32)
    lane_group = lax.shift_right_logical(iota((N_ROWS, 128), 1), 3)
    xrow[...] = jnp.where(lane_group == lax.rem(r + 1, 16), loss_here, ordered)
    for d in range(N_ROWS):
        sbuf[d] = xrow[d:d + 1, :]
    rbuf[r] = xrow[pl.ds(r, 1), :]
    def send_rows():
        for i in range(1, N_ROWS):
            to = row_at(i // NX, i % NX)
            pltpu.make_async_remote_copy(
                sbuf.at[to], rbuf.at[r], os_, or_,
                device_id={"rows": to}, device_id_type=MESH).start()

    one = jnp.where(r < N_ROWS, 1.0, 0.0)
    sums = {p: [None, None] for p in range(4)}

    def tiles(p, first, last):
        for t in range(first, last):
            left = []
            for u in range(2):
                k = 2 * t + u
                q16 = jnp.broadcast_to(qrow[k:k + 1, :], (16, PAIRS)).astype(I16)
                c16 = jnp.broadcast_to(coef[k:k + 1, :], (16, PAIRS)).astype(BF)
                q16 = jnp.concatenate([q16] * 8, axis=0)
                c16 = jnp.concatenate([c16] * 8, axis=0)
                hit = q16 == iota((128, PAIRS), 0, I16) + jnp.int16(128 * p)
                left.append(jnp.where(hit, c16, jnp.zeros((), BF)))
            rows = pl.ds(t * 2 * PAIRS, 2 * PAIRS)
            d = jnp.dot(jnp.concatenate(left, axis=1), vx[rows, :], preferred_element_type=F32)
            sums[p][t % 2] = d if sums[p][t % 2] is None else sums[p][t % 2] + d

    def send_piece(p):
        total = sums[p][0] + sums[p][1] * one
        for h in range(2):
            for c in range(NX):
                block = total[c * 32:c * 32 + 32, 128 * h:128 * h + 128]
                if c == 0 and (p in SUMMED or p == 0 and h == 0):
                    kept[p, h] = block
                else:
                    gsend[p, c, h] = block.astype(BF)
        if p in SUMMED:
            for dx in (2, 1, 3):
                pltpu.make_async_remote_copy(
                    gsend.at[p, dx], grecv.at[p, dx], gs.at[p], gr.at[p],
                    device_id={"rows": row_at(0, dx)}, device_id_type=MESH).start()
            return
        for dx in (2, 1, 3, 0):
            for dz in (4, 3, 5, 2, 6, 1, 7, 0):
                s, h, j, c = place(dz, dx)
                if 2 * s + j == p and (dz != 0 or dx != 0):
                    pltpu.make_async_remote_copy(
                        gsend.at[p, c, h], grecv.at[p, c, h], gs.at[p], gr.at[p],
                        device_id={"rows": row_at(dz, dx)}, device_id_type=MESH).start()

    def along_z(p):
        all_of(gsend.at[p, pl.ds(1, NX - 1)], gs.at[p], gr.at[p]).wait_recv()
        for h in range(2):
            block = kept[p, h]
            for dx in range(1, NX):
                block = block + grecv[p, dx, h].astype(F32)
            gsend[p, 0, h] = block.astype(BF)
        for dz in (4, 3, 5, 2):
            s, h, j, _ = place(dz, 0)
            if 2 * s + j == p:
                pltpu.make_async_remote_copy(
                    gsend.at[p, 0, h], grecv.at[p, 0, h], fs, fr,
                    device_id={"rows": row_at(dz, 0)}, device_id_type=MESH).start()

    count = PAIRS // 2
    tiles(2, 0, count)
    tiles(3, 0, LAG)
    send_piece(2)
    tiles(3, LAG, count)
    tiles(1, 0, LAG)
    send_piece(3)
    send_rows()
    tiles(1, LAG, count)
    tiles(0, 0, LAG)
    send_piece(1)
    tiles(0, LAG, ZTILE)
    along_z(2)
    tiles(0, ZTILE, count)
    send_piece(0)
    if 3 in SUMMED:
        along_z(3)

    all_of(rbuf.at[pl.ds(0, N_ROWS - 1)], os_, or_).wait_recv()
    group1 = lax.shift_right_logical(iota((1, 128), 1), 3)
    loss_sum = jnp.zeros((1, 128), F32)
    for h in range(2):
        mine = jnp.zeros((1, 128), F32)
        for g in range(16):
            row = rbuf[h * 16 + g]
            mine = mine + jnp.where(group1 == g, row, 0.0)
            loss_sum = loss_sum + jnp.where(group1 == (g + 1) % 16, row, 0.0)
        own_out[pl.ds(h, 1), :] = mine
    loss_total = jnp.sum(loss_sum, axis=1, keepdims=True) * (1.0 / (8.0 * 8192.0))
    loss_out[...] = jnp.broadcast_to(loss_total, (1, 128))

    total = kept[0, 0]
    for p in (3, 1, 2, 0):
        if p in SUMMED:
            continue
        first = 0 if p else 1
        all_of(vx.at[pl.ds(0, (8 - first) * 16)], gs.at[p], gr.at[p]).wait_recv()
        for n in range(first, 8):
            total = total + grecv[p, n // 2, n % 2].astype(F32)
    all_of(vx.at[pl.ds(0, 2 * len(SUMMED) * 16)], fs, fr).wait_recv()
    for p in SUMMED:
        for h in range(2):
            total = total + grecv[p, 0, h].astype(F32)
    grad_out[...] = total

    all_of(vx.at[pl.ds(0, 4 * 16)], zs, zr.at[0]).wait_send()
    all_of(vx.at[pl.ds(0, 27 * 16)], xs, xr.at[0]).wait_send()
    all_of(mbuf.at[pl.ds(0, N_FEAT - 1)], ms, mr).wait_send()
    all_of(sbuf.at[pl.ds(0, N_ROWS - 1)], os_, or_).wait_send()
    for p in range(4):
        sent = 6 if p in SUMMED else 8 if p else 7
        all_of(vx.at[pl.ds(0, sent * 16)], gs.at[p], gr.at[p]).wait_send()
    all_of(vx.at[pl.ds(0, 2 * len(SUMMED) * 16)], fs, fr).wait_send()


def finish(own_in, grad_in, loss_in, own_out, grad_out, loss_out):
    own_out[...] = own_in[...]
    grad_out[...] = grad_in[...]
    loss_out[...] = loss_in[...]


def on_device(tile_values, tile_blocks, tile_counts, labels, owner_rank, weights):
    vmem = pl.BlockSpec(memory_space=pltpu.VMEM)
    dma = pltpu.SemaphoreType.DMA
    results = (
        jax.ShapeDtypeStruct((2, 128), F32),
        jax.ShapeDtypeStruct((32, 128), F32),
        jax.ShapeDtypeStruct((1, 128), F32),
    )
    parts = pl.pallas_call(
        body,
        out_shape=results,
        in_specs=[pl.BlockSpec(memory_space=pl.ANY)] * 6,
        out_specs=(vmem, vmem, vmem),
        scratch_shapes=[
            pltpu.VMEM((64, 256), I32),
            pltpu.VMEM((1, 256), I32),
            pltpu.VMEM((2, 128), I32),
            pltpu.VMEM((2, 128), I32),
            pltpu.VMEM((32, 128), F32),
            pltpu.VMEM((256, 64, 128), BF),
            pltpu.VMEM((16384, 256), BF),
            pltpu.VMEM((2, 16384, 256), BF),
            pltpu.VMEM((2, PAIRS * 8, 128), F32),
            pltpu.VMEM((2, 2, 2, NX, 32, 128), BF),
            pltpu.VMEM((PAIRS, PAIRS), I32),
            pltpu.VMEM((PAIRS, PAIRS), I32),
            pltpu.VMEM((PAIRS, PAIRS), F32),
            pltpu.VMEM((256, 128), BF),
            pltpu.VMEM((N_FEAT, 2, 128), F32),
            pltpu.VMEM((N_ROWS, 1, 128), F32),
            pltpu.VMEM((N_ROWS, 1, 128), F32),
            pltpu.VMEM((N_ROWS, 128), F32),
            pltpu.VMEM((4, 2, 32, 128), F32),
            pltpu.VMEM((4, NX, 2, 32, 128), BF),
            pltpu.VMEM((4, NX, 2, 32, 128), BF),
            dma((5,)), dma((VCHUNKS,)),
            dma, dma((NZ,)),
            dma, dma((3,)),
            dma, dma,
            dma, dma,
            dma((4,)), dma((4,)),
            dma, dma,
        ],
        compiler_params=pltpu.CompilerParams(
            collective_id=0, has_side_effects=True, vmem_limit_bytes=40 * 1024 * 1024),
    )(*[pltpu.with_memory_space_constraint(a, pltpu.HBM) for a in (tile_blocks.T, tile_counts.T, labels.reshape(2, 128), owner_rank.reshape(2, 128), weights, tile_values)])
    own, grad, loss = pl.pallas_call(
        finish, out_shape=results, in_specs=[vmem] * 3, out_specs=(vmem, vmem, vmem),
        compiler_params=pltpu.CompilerParams(vmem_limit_bytes=1024 * 1024),
    )(*parts)
    return own.reshape(256), grad, loss[0, 0]


def solution(mesh):
    in_specs = (
        P("rows", "feat", None),
        P("rows", "feat"),
        P("rows", "feat"),
        P("rows"),
        P("rows"),
        P(("feat", "rows"), None),
    )
    out_specs = (P("rows"), P(("feat", "rows"), None), P())
    return jax.shard_map(
        on_device, mesh=mesh, in_specs=in_specs, out_specs=out_specs, check_vma=False
    )
```
